32 devices in a mesh: clip: 2 (over core), ha: 4 (over y, x), wa: 4 (over z).
Axes of the slice: x: 2, y: 2, z: 4, core: 2. Of those that a mesh axis runs over, the one named last changes fastest.
Arguments:
- frames: bfloat16 [8, 96, 128, 128], P('clip', 'ha', 'wa'), parts along dimension 0, may hold values from -60 to 60, as said below
- caches: bfloat16 [4, 4, 96, 128, 128], P('clip', None, 'ha', 'wa'), parts along dimension 0, may hold values from -4 to 4
- conv_weights: bfloat16 [4, 3, 3, 3, 128, 128], replicated, may hold values from -0.109375 to 0.109375
- conv_bias: float32 [4, 128], replicated, may hold values from -3 to 3
- norm_gain: float32 [4, 128], replicated, may hold values from 0.25 to 1.75
- norm_shift: float32 [4, 128], replicated, may hold values from -3 to 3
Outputs:
- encoded: bfloat16 [8, 96, 128, 128], P('clip', 'ha', 'wa'), parts along dimension 0
- new_caches: bfloat16 [4, 4, 96, 128, 128], P('clip', None, 'ha', 'wa'), parts along dimension 0
The draws below stay inside these ranges and needn't reach their ends.
There are 2 independent parts, one for each index of `clip`. The reference program is written for one: setup_inputs(seed, part) draws one part's arguments, and reference() takes and returns one part's arrays. A program takes and returns all parts, laid end to end along the dimension named above; an argument that names none is the same for every part. Nothing has to cross between parts.
Inputs may be any that keep to these rules, and one draw needn't show every extreme that they name: `frames`: real-valued features.
All inputs are finite; a program needn't handle non-finite values.
Results may differ from the reference program's by a relative error of at most 0.005.
Values may be sent and summed in bfloat16 or wider, within the bound.
A program may use at most 64 MiB of HBM per device.

```python
import jax
import jax.numpy as jnp
from jax import lax

C = 128
GROUPS = 32
FR = 4
BLOCKS = 2
CACHE = 2
CONVS = 4
H = 96
W = 128


def draw_frames(key, part):
    streams = jax.random.split(jax.random.fold_in(key, 11), 3)
    row_pos = jnp.arange(H, dtype=jnp.float32) / (H - 1)
    col_pos = jnp.arange(W, dtype=jnp.float32) / (W - 1)
    trend = jnp.log(0.5) + jnp.log(3.0) * 0.5 * (row_pos[:, None] + col_pos[None, :])
    cell_level = jax.random.uniform(streams[0], (FR, H, W, 1), jnp.float32, -1.15, 1.15)
    channel_level = jnp.exp(jax.random.uniform(streams[1], (C,), jnp.float32, -1.15, 1.15))
    noise = jnp.clip(jax.random.normal(streams[2], (FR, H, W, C), jnp.float32), -3.0, 3.0)
    values = jnp.exp(trend[None, :, :, None] + cell_level) * channel_level * noise
    return values.astype(jnp.bfloat16)


def block_scale(stream_key, dims, pieces, low, high):
    factor_of = 1.0
    for dim, shards_of in pieces:
        heights = jax.random.uniform(jax.random.fold_in(jax.random.fold_in(stream_key, 6), dim), (shards_of,), jnp.float32, low / len(pieces), high / len(pieces))
        factor_of = factor_of * jnp.repeat(jnp.exp(heights), dims[dim] // shards_of).reshape((-1,) + (1,) * (len(dims) - 1 - dim))
    return factor_of


def gaussian(key, shape, spread, most, cuts=(), held_as=jnp.bfloat16):
    values = spread * jax.random.normal(key, shape, jnp.float32)
    if cuts:
        values = values * block_scale(key, shape, cuts, -0.22, 0.18)
    return jnp.clip(values, -most, most).astype(held_as)


def setup_inputs(seed: int = 0, part: int = 0) -> dict:
    keys = jax.random.split(jax.random.key(seed), 7)
    part_keys = jax.random.split(jax.random.fold_in(keys[6], part), 7)
    frames = draw_frames(jax.random.fold_in(jax.random.fold_in(keys[6], part), 71), part)
    caches = gaussian(part_keys[1], (CACHE, CONVS, H, W, C), 1.0, 4.0, ((2, 4), (3, 4)))
    conv_weights = gaussian(keys[2], (CONVS, 3, 3, 3, C, C), (27 * C) ** -0.5, 0.109375)
    conv_bias = gaussian(keys[3], (CONVS, C), 0.5, 3.0, (), jnp.float32)
    norm_gain = jnp.clip(1.0 + 0.15 * jax.random.normal(keys[4], (CONVS, C), jnp.float32), 0.25, 1.75)
    norm_shift = gaussian(keys[5], (CONVS, C), 0.5, 3.0, (), jnp.float32)
    return {"frames": frames, "caches": caches, "conv_weights": conv_weights, "conv_bias": conv_bias, "norm_gain": norm_gain, "norm_shift": norm_shift}


EPSILON = 1e-06

def group_norm(values, gain_row, shift_row):
    grouped = values.reshape(values.shape[0], values.shape[1], values.shape[2], GROUPS, -1)
    group_mean = lax.optimization_barrier(jnp.mean(grouped, axis=(0, 1, 2, 4), keepdims=True))
    centered = grouped - group_mean
    variance = lax.optimization_barrier(jnp.mean(centered * centered, axis=(0, 1, 2, 4), keepdims=True))
    normed = centered / jnp.sqrt(variance + EPSILON)
    return normed.reshape(values.shape) * gain_row + shift_row

def causal_conv(activation, history, kernel, bias_row):
    joined = jnp.concatenate([history, activation], axis=0).astype(jnp.float32)
    padded = jnp.pad(joined, ((0, 0), (1, 1), (1, 1), (0, 0)))
    result = lax.conv_general_dilated(padded[None], kernel.astype(jnp.float32), (1, 1, 1), 'VALID', dimension_numbers=('NDHWC', 'DHWIO', 'NDHWC'), precision=lax.Precision.HIGHEST)
    return result[0] + bias_row

def reference(frames, caches, conv_weights, conv_bias, norm_gain, norm_shift):
    block_input = frames
    saved = []
    for block_index in range(BLOCKS):
        first_conv = 2 * block_index
        second_conv = first_conv + 1
        first_act = jax.nn.silu(group_norm(block_input.astype(jnp.float32), norm_gain[first_conv], norm_shift[first_conv])).astype(jnp.bfloat16)
        saved.append(first_act[FR - CACHE:])
        middle = causal_conv(first_act, caches[:, first_conv], conv_weights[first_conv], conv_bias[first_conv])
        second_act = jax.nn.silu(group_norm(middle, norm_gain[second_conv], norm_shift[second_conv])).astype(jnp.bfloat16)
        saved.append(second_act[FR - CACHE:])
        branch = causal_conv(second_act, caches[:, second_conv], conv_weights[second_conv], conv_bias[second_conv])
        block_input = (block_input.astype(jnp.float32) + branch).astype(jnp.bfloat16)
    return (block_input, jnp.stack(saved, axis=1))
```

```python
import functools

import jax
import jax.numpy as jnp
from jax import lax
from jax.experimental import pallas as pl
from jax.experimental.pallas import tpu as pltpu
from jax.sharding import PartitionSpec as P

GROUPS = 32
EPSILON = 1e-06
MESH = pl.DeviceIdType.MESH
F32 = jnp.float32
BF16 = jnp.bfloat16
DIRECTIONS = [(dy, dx) for dy in (-1, 0, 1) for dx in (-1, 0, 1) if (dy, dx) != (0, 0)]
SIDE = (-1, 1)
LEAD = 8
POINTS = 4
PLANES = 4


def silu_of_half(half):
    return half + half * jnp.tanh(half)


def exists_at(nh, nw):
    ha, wa = lax.axis_index("ha"), lax.axis_index("wa")

    def exists(dy, dx):
        conds = []
        if dy:
            conds.append(ha > 0 if dy < 0 else ha < nh - 1)
        if dx:
            conds.append(wa > 0 if dx < 0 else wa < nw - 1)
        return conds[0] if len(conds) == 1 else jnp.logical_and(*conds)

    return exists


def build(s, d, h, w, c, row_of, rows, cols, ends):
    pitch = w + 2 * LEAD
    half = w // 2
    for r in range(h + 2):
        cells = rows[0]() if r == 0 else rows[1]() if r == h + 1 else row_of(r - 1)
        at = r * pitch + LEAD
        s[at : at + w, :] = cells
    for side in range(2):
        edge = LEAD - 1 + side * (w + 1)
        s[pl.ds(pitch + edge, h, stride=pitch), :] = cols[side]()
        for low in range(2):
            at = low * (h + 1) * pitch + edge
            s[at : at + 1, :] = ends[low * 2 + side]()

    def planes(r):
        return [
            s[pl.ds(r * pitch + LEAD - 1 + j, half, stride=2), :] for j in range(PLANES)
        ]

    window = [planes(0), planes(1)]
    for i in range(h // 2):
        window = window[-2:] + [planes(2 * i + 2), planes(2 * i + 3)]
        for j in range(PLANES):
            r0, r1, r2, r3 = (row[j] for row in window)
            for point, value in enumerate((r2 - r0, r1 + r2, r1 - r2, r1 - r3)):
                d[point, j, i * half : (i + 1) * half, :] = value.astype(BF16)


def taps(t, low, high):
    return lambda point: t[point, low:high].reshape(-1, t.shape[-1])


def products(pieces, right):
    m = []
    for point in range(POINTS):
        left = jnp.concatenate([p[point, j] for p in pieces for j in range(PLANES)], axis=1)
        m.append(jnp.dot(left, right(point), preferred_element_type=F32))
    return (m[1] - m[2]) - m[0], m[1] - (m[3] - m[2])


def live_phase(dims, odd, exists, multiplier, offset, bias_row, source, target, res, halos, s, d, t, acc, kept, emit):
    fr, cf, h, w, c = dims
    half = w // 2
    hr, hc, hk = halos
    multiplier, offset = 0.5 * multiplier, 0.5 * offset

    def act(values):
        return silu_of_half(values * multiplier + offset).astype(BF16)

    def masked(dy, dx, values):
        return jnp.where(exists(dy, dx), values.astype(F32), 0.0)

    def build_frame(f):
        def row_of(r):
            cells = act(source[f, r * w : (r + 1) * w, :])
            if f >= fr - cf:
                kept[f - (fr - cf), r * w : (r + 1) * w, :] = cells
            return cells.astype(F32)

        build(
            s.at[f],
            d.at[f],
            h,
            w,
            c,
            row_of,
            [lambda i=i: masked(SIDE[i], 0, act(hr[i, f].astype(F32))) for i in range(2)],
            [lambda i=i: masked(0, SIDE[i], act(hc[i, f].astype(F32))) for i in range(2)],
            [lambda i=i: masked(SIDE[i // 2], SIDE[i % 2], act(hk[i, f])) for i in range(4)],
        )

    zero = jnp.zeros((8, c), F32)
    sums, squares = zero, zero
    build_frame(0)
    for o in range(fr):
        first = max(0, o - cf)
        dt = first + cf - o
        both = products(
            [d.at[f] for f in range(first, o + 1)],
            taps(t, dt, cf + 1),
        )
        if o + 1 < fr:
            build_frame(o + 1)
        for q in range(2):
            y = both[q]
            if o < cf:
                y = y + acc[o, q]
            for i in range(h // 2):
                for e in range(2):
                    piece = y[i * half : (i + 1) * half, e * c : (e + 1) * c] + bias_row
                    at = pl.ds((2 * i + q) * w + e, half, stride=2)
                    if odd:
                        piece = (res[o, at, :] + piece).astype(BF16).astype(F32)
                    target[o, at, :] = piece
                    if emit is None:
                        slabs = piece.reshape(half // 8, 8, c)
                        sums = sums + jnp.sum(slabs, axis=0)
                        squares = squares + jnp.sum(slabs * slabs, axis=0)
        if emit is not None:
            emit(o)
    return sums, squares


def kernel(dims, *refs):
    (frames, caches, weights, bias_in, gain_in, shift_in,
     mid, res, acc, t_last, norm, hr_last, hc_last, hk_last, kept,
     x, cb, wv, s, d, dc, t, small,
     s_out, s_in,
     lr_out, lc_out, lk_out, lr_in, lc_in, lk_in,
     cr_out, cc_out, ck_out, cr_in, cc_in, ck_in,
     load_sem, weight_sem, small_sem,
     stat_send, stat_recv, halo_send, halo_recv) = refs
    nh, nw, fr, cf, convs, h, w, c = dims
    peers = nh * nw
    cell_count = fr * h * w * peers * (c // GROUPS)
    clip, ha, wa = lax.axis_index("clip"), lax.axis_index("ha"), lax.axis_index("wa")
    offsets = [(i, j) for i in range(nh) for j in range(nw) if (i, j) != (0, 0)]
    others = [(lax.rem(ha + i, nh), lax.rem(wa + j, nw)) for i, j in offsets]
    exists = exists_at(nh, nw)
    barrier = pltpu.get_barrier_semaphore()
    for ph, pw in others:
        pl.semaphore_signal(barrier, inc=1, device_id=(clip, ph, pw), device_id_type=MESH)

    load_x = pltpu.make_async_copy(frames, x, load_sem.at[0])
    load_x.start()

    def span(k):
        return pl.ds(0, 1) if k == 0 else pl.ds(1, convs - 1)

    def load_cache(k):
        return pltpu.make_async_copy(caches.at[:, span(k)], cb.at[:, span(k)], load_sem.at[1 + k])

    def load_weights(k):
        return pltpu.make_async_copy(weights.at[span(k)], wv.at[span(k)], weight_sem.at[k])

    small_copies = [
        pltpu.make_async_copy(ref, small.at[i], small_sem.at[i])
        for i, ref in enumerate((bias_in, gain_in, shift_in))
    ]
    for copy in small_copies:
        copy.start()
    for k in range(2):
        load_cache(k).start()
        load_weights(k).start()
    bias, gain, shift = small.at[0], small.at[1], small.at[2]

    def halo_copy(live, k, dy, dx, towards):
        inbox = (1, 3)[k % 2] if live else (0, 2)[k]
        outbox = int(live)
        group = span(k)
        rows_out, rows_in = (lr_out, lr_in) if live else (cr_out, cr_in)
        cols_out, cols_in = (lc_out, lc_in) if live else (cc_out, cc_in)
        ends_out, ends_in = (lk_out, lk_in) if live else (ck_out, ck_in)
        if dx == 0:
            src, dst = rows_out, rows_in
            near, far = int(dy > 0), int(dy < 0)
        elif dy == 0:
            src, dst = cols_out, cols_in
            near, far = int(dx > 0), int(dx < 0)
        else:
            src, dst = ends_out, ends_in
            near = int(dy > 0) * 2 + int(dx > 0)
            far = 3 - near
        if live:
            src, dst = src.at[k, near], dst.at[k, far]
        else:
            src, dst = src.at[near, group], dst.at[far, group]
        direction = DIRECTIONS.index((dy, dx))
        back = DIRECTIONS.index((-dy, -dx))
        return pltpu.make_async_remote_copy(
            src_ref=src,
            dst_ref=dst,
            send_sem=halo_send.at[outbox, direction],
            recv_sem=halo_recv.at[inbox, back],
            device_id=(clip, ha + dy * towards, wa + dx * towards),
            device_id_type=MESH,
        )

    def pack_edges(k, field):
        for f in range(fr):
            for side in range(2):
                first = side * (w - 1)
                top = side * (h - 1) * w
                lr_out[k, side, f] = field[f, top : top + w, :].astype(BF16)
                lc_out[k, side, f] = field[f, pl.ds(first, h, stride=w), :].astype(BF16)
                for low in range(2):
                    row = low * (h - 1) * w + first
                    lk_out[k, low * 2 + side, f] = field[f, row : row + 1, :]

    def send_halo(live, k):
        for dy, dx in DIRECTIONS:

            @pl.when(exists(dy, dx))
            def _():
                halo_copy(live, k, dy, dx, 1).start()

    def wait_halo(live, k):
        for dy, dx in DIRECTIONS:

            @pl.when(exists(dy, dx))
            def _():
                halo_copy(live, k, -dy, -dx, -1).wait_recv()

    def wait_sent(live, k):
        for dy, dx in DIRECTIONS:

            @pl.when(exists(dy, dx))
            def _():
                halo_copy(live, k, dy, dx, 1).wait_send()

    def send_stats(k, sums, squares):
        s_out[k] = jnp.concatenate(
            [jnp.sum(sums, axis=0, keepdims=True), jnp.sum(squares, axis=0, keepdims=True)], axis=0
        )
        for number, (ph, pw) in enumerate(others):
            pltpu.make_async_remote_copy(
                src_ref=s_out.at[k],
                dst_ref=s_in.at[k, number],
                send_sem=stat_send.at[0],
                recv_sem=stat_recv.at[k % 2],
                device_id=(clip, ph, pw),
                device_id_type=MESH,
            ).start()

    def all_stats(k, sem):
        return pltpu.make_async_copy(s_in.at[k], s_in.at[k], sem)

    def wait_stats(k):
        all_stats(k, stat_recv.at[k % 2]).wait()
        parts = [s_out[k]] + [s_in[k, i] for i in range(peers - 1)]
        while len(parts) > 1:
            parts = [
                parts[i] + parts[i + 1] if i + 1 < len(parts) else parts[i]
                for i in range(0, len(parts), 2)
            ]
        total = jnp.concatenate([parts[0], jnp.zeros((6, c), F32)], axis=0)
        lane = lax.broadcasted_iota(jnp.int32, (8, c), 1)
        step = 1
        while step < c // GROUPS:
            total = total + jnp.where(
                lax.rem(lane, 2 * step) < step,
                pltpu.roll(total, c - step, 1),
                pltpu.roll(total, step, 1),
            )
            step *= 2
        mean = total[0:1] / cell_count
        variance = total[1:2] / cell_count - mean * mean
        multiplier = lax.rsqrt(variance + EPSILON) * gain[k : k + 1, :]
        offset = shift[k : k + 1, :] - mean * multiplier
        return multiplier, offset

    def table(k):
        return t_last if k == convs - 1 else t.at[k % 2]

    def transform_weights(k):
        if k < 2:
            load_weights(k).wait()
        into = table(k)

        def body(dt, carry):
            for dw in range(3):
                rows = slice(dw * c, (dw + 1) * c)
                g = [wv[k, dt, dh, rows, :] for dh in range(3)]
                outer = g[0].astype(F32) + g[2].astype(F32)
                inner = g[1].astype(F32)
                values = (
                    g[0],
                    (0.5 * (outer + inner)).astype(BF16),
                    (0.5 * (outer - inner)).astype(BF16),
                    g[2],
                )
                for point in range(POINTS):
                    for e in range(2):
                        j = dw + e
                        into[point, dt, j * c : (j + 1) * c, e * c : (e + 1) * c] = values[point]
            for point in range(POINTS):
                into[point, dt, 3 * c : 4 * c, 0:c] = jnp.zeros((c, c), BF16)
                into[point, dt, 0:c, c : 2 * c] = jnp.zeros((c, c), BF16)
            return carry

        lax.fori_loop(0, 3, body, 0)

    def masked(dy, dx, values):
        return jnp.where(exists(dy, dx), values, 0.0)

    def cached_phase(k):
        for f in range(cf):
            build(
                s.at[f],
                dc.at[f],
                h,
                w,
                c,
                lambda r: cb[f, k, r * w : (r + 1) * w, :].astype(F32),
                [lambda i=i: masked(SIDE[i], 0, cr_in[i, k, f].astype(F32)) for i in range(2)],
                [lambda i=i: masked(0, SIDE[i], cc_in[i, k, f].astype(F32)) for i in range(2)],
                [lambda i=i: masked(SIDE[i // 2], SIDE[i % 2], ck_in[i, k, f]) for i in range(4)],
            )
        into = table(k)
        for o in range(cf):
            both = products(
                [dc.at[p] for p in range(o, cf)],
                taps(into, 0, cf - o),
            )
            for q in range(2):
                acc[o, q] = both[q]

    def pack_cached(k):
        if k < 2:
            load_cache(k).wait()

        for f in range(cf):
            for side in range(2):
                top = side * (h - 1) * w
                cr_out[side, k, f] = cb[f, k, top : top + w, :]
                s[f, 0 : h * w, :] = cb[f, k].astype(F32)
                first = side * (w - 1)
                cc_out[side, k, f] = s[f, pl.ds(first, h, stride=w), :].astype(BF16)
                for low in range(2):
                    row = low * (h - 1) * w + first
                    ck_out[low * 2 + side, k, f] = s[f, row : row + 1, :]

    def settle(k):
        wait_sent(True, k)
        all_stats(k, stat_send.at[0]).wait()

    load_x.wait()

    def widen(f, carry):
        sums, squares = carry
        values = x[f].astype(F32)
        res[f] = values
        slabs = values.reshape(h * w // 8, 8, c)
        return sums + jnp.sum(slabs, axis=0), squares + jnp.sum(slabs * slabs, axis=0)

    zero = jnp.zeros((8, c), F32)
    carry = lax.fori_loop(0, fr, widen, (zero, zero))
    pack_edges(0, res)
    pack_cached(0)
    pl.semaphore_wait(barrier, peers - 1)
    send_stats(0, *carry)
    send_halo(False, 0)
    transform_weights(0)
    send_halo(True, 0)
    for k in range(1, convs):
        pack_cached(k)
    wait_halo(False, 0)
    cached_phase(0)
    for copy in small_copies:
        copy.wait()
    last = convs - 1
    for k in range(convs):
        multiplier, offset = wait_stats(k)
        wait_halo(True, k)
        if k == last:
            break
        if k == 0:
            wait_sent(False, 0)
            send_halo(False, 1)
        source, target = (mid, res) if k % 2 else (res, mid)
        carry = live_phase(
            (fr, cf, h, w, c), k % 2, exists, multiplier, offset, bias[k : k + 1, :],
            source, target, res, (lr_in.at[k], lc_in.at[k], lk_in.at[k]),
            s, d, table(k), acc, kept.at[k], None,
        )
        settle(k)
        send_stats(k + 1, *carry)
        pack_edges(k + 1, target)
        send_halo(True, k + 1)
        transform_weights(k + 1)
        if k == 0:
            wait_halo(False, 1)
        cached_phase(k + 1)
        if k == 0:
            wait_sent(False, 1)

    norm[...] = jnp.zeros_like(norm)
    norm[0:1] = multiplier
    norm[1:2] = offset
    norm[2:3] = bias[last : last + 1, :]
    hr_last[...] = lr_in[last]
    hc_last[...] = lc_in[last]
    hk_last[...] = lk_in[last]
    settle(last)


def finish(dims, *refs):
    (mid, res, acc, t_last, norm_last, hr, hc, hk, kept,
     encoded, new_caches,
     s, d, out, kept_new, y, out_sem, kept_sem) = refs
    nh, nw, fr, cf, convs, h, w, c = dims
    exists = exists_at(nh, nw)
    copies = [
        pltpu.make_async_copy(kept.at[k], new_caches.at[:, k], kept_sem.at[k])
        for k in range(convs - 1)
    ]
    for copy in copies:
        copy.start()

    def emit(o):
        out[o] = y[o].astype(BF16)

    live_phase(
        (fr, cf, h, w, c), (convs - 1) % 2, exists, norm_last[0:1], norm_last[1:2], norm_last[2:3],
        mid, y, res, (hr, hc, hk), s, d, t_last, acc, kept_new, emit,
    )
    copies.append(
        pltpu.make_async_copy(kept_new, new_caches.at[:, convs - 1], kept_sem.at[convs - 1])
    )
    copies[-1].start()
    copies.append(pltpu.make_async_copy(out, encoded, out_sem.at[0]))
    copies[-1].start()
    for copy in copies:
        copy.wait()


def local(nh, nw, frames, caches, conv_weights, conv_bias, norm_gain, norm_shift):
    fr, h, w, c = frames.shape
    cf, convs = caches.shape[:2]
    dims = (nh, nw, fr, cf, convs, h, w, c)
    peers = nh * nw
    vmem = pltpu.VMEM
    dma = pltpu.SemaphoreType.DMA
    pitch = w + 2 * LEAD
    pairs = h * w // 4
    s_shape = vmem((fr, (h + 2) * pitch, c), F32)
    d_shape = vmem((fr, POINTS, PLANES, pairs, c), BF16)
    table = (POINTS, cf + 1, PLANES * c, 2 * c)
    scratch = [
        vmem((fr, h * w, c), BF16),
        vmem((cf, convs, h * w, c), BF16),
        vmem((convs, 3, 3, 3 * c, c), BF16),
        s_shape,
        d_shape,
        vmem((cf, POINTS, PLANES, pairs, c), BF16),
        vmem((2,) + table, BF16),
        vmem((3, convs, c), F32),
        vmem((convs, 2, c), F32),
        vmem((convs, peers - 1, 2, c), F32),
    ]
    for _ in range(2):
        scratch += [
            vmem((convs, 2, fr, w, c), BF16),
            vmem((convs, 2, fr, h, c), BF16),
            vmem((convs, 4, fr, 1, c), F32),
        ]
    for _ in range(2):
        scratch += [
            vmem((2, convs, cf, w, c), BF16),
            vmem((2, convs, cf, h, c), BF16),
            vmem((4, convs, cf, 1, c), F32),
        ]
    scratch += [
        dma((3,)),
        dma((2,)),
        dma((3,)),
        dma((1,)),
        dma((2,)),
        dma((2, 8)),
        dma((4, 8)),
    ]
    anywhere = pl.BlockSpec(memory_space=pltpu.HBM)
    inside = pl.BlockSpec(memory_space=pltpu.VMEM)
    handed = [
        ((fr, h * w, c), F32),
        ((fr, h * w, c), F32),
        ((cf, 2, pairs, 2 * c), F32),
        (table, BF16),
        ((8, c), F32),
        ((2, fr, w, c), BF16),
        ((2, fr, h, c), BF16),
        ((4, fr, 1, c), F32),
        ((convs - 1, cf, h * w, c), BF16),
    ]
    state = pl.pallas_call(
        functools.partial(kernel, dims),
        out_shape=[vmem(shape, dtype) for shape, dtype in handed],
        in_specs=[anywhere] * 6,
        out_specs=[inside] * len(handed),
        scratch_shapes=scratch,
        compiler_params=pltpu.CompilerParams(
            collective_id=0, has_side_effects=True, vmem_limit_bytes=48 * 1024 * 1024
        ),
    )(
        frames.reshape(fr, h * w, c),
        caches.reshape(cf, convs, h * w, c),
        conv_weights.reshape(convs, 3, 3, 3 * c, c),
        conv_bias,
        norm_gain,
        norm_shift,
    )
    encoded, new_caches = pl.pallas_call(
        functools.partial(finish, dims),
        out_shape=(
            jax.ShapeDtypeStruct((fr, h * w, c), BF16),
            jax.ShapeDtypeStruct((cf, convs, h * w, c), BF16),
        ),
        in_specs=[inside] * len(handed),
        out_specs=(anywhere, anywhere),
        scratch_shapes=[
            s_shape,
            d_shape,
            vmem((fr, h * w, c), BF16),
            vmem((cf, h * w, c), BF16),
            vmem((fr, h * w, c), F32),
            dma((1,)),
            dma((convs,)),
        ],
        compiler_params=pltpu.CompilerParams(vmem_limit_bytes=24 * 1024 * 1024),
    )(*state)
    return encoded.reshape(frames.shape), new_caches.reshape(caches.shape)


def solution(mesh):
    return jax.shard_map(
        functools.partial(local, mesh.shape["ha"], mesh.shape["wa"]),
        mesh=mesh,
        in_specs=(
            P("clip", "ha", "wa", None),
            P("clip", None, "ha", "wa", None),
            P(),
            P(),
            P(),
            P(),
        ),
        out_specs=(P("clip", "ha", "wa", None), P("clip", None, "ha", "wa", None)),
        check_vma=False,
    )
```

```python
import functools

import jax
import jax.numpy as jnp
from jax import lax
from jax.experimental import pallas as pl
from jax.experimental.pallas import tpu as pltpu
from jax.sharding import PartitionSpec as P

GROUPS = 32
EPSILON = 1e-06
MESH = pl.DeviceIdType.MESH
F32 = jnp.float32
BF16 = jnp.bfloat16
DIRECTIONS = [(dy, dx) for dy in (-1, 0, 1) for dx in (-1, 0, 1) if (dy, dx) != (0, 0)]
SIDE = (-1, 1)
LEAD = 8
POINTS = 4
PLANES = 4


def silu_of_half(half):
    return half + half * jnp.tanh(half)


def exists_at(nh, nw):
    ha, wa = lax.axis_index("ha"), lax.axis_index("wa")

    def exists(dy, dx):
        conds = []
        if dy:
            conds.append(ha > 0 if dy < 0 else ha < nh - 1)
        if dx:
            conds.append(wa > 0 if dx < 0 else wa < nw - 1)
        return conds[0] if len(conds) == 1 else jnp.logical_and(*conds)

    return exists


def build(s, d, h, w, c, row_of, rows, cols, ends):
    pitch = w + 2 * LEAD
    half = w // 2
    for r in range(h + 2):
        cells = rows[0]() if r == 0 else rows[1]() if r == h + 1 else row_of(r - 1)
        at = r * pitch + LEAD
        s[at : at + w, :] = cells
    for side in range(2):
        edge = LEAD - 1 + side * (w + 1)
        s[pl.ds(pitch + edge, h, stride=pitch), :] = cols[side]()
        for low in range(2):
            at = low * (h + 1) * pitch + edge
            s[at : at + 1, :] = ends[low * 2 + side]()

    def planes(r):
        return [
            s[pl.ds(r * pitch + LEAD - 1 + j, half, stride=2), :] for j in range(PLANES)
        ]

    window = [planes(0), planes(1)]
    for i in range(h // 2):
        window = window[-2:] + [planes(2 * i + 2), planes(2 * i + 3)]
        for j in range(PLANES):
            r0, r1, r2, r3 = (row[j] for row in window)
            for point, value in enumerate((r2 - r0, r1 + r2, r1 - r2, r1 - r3)):
                d[point, j, i * half : (i + 1) * half, :] = value.astype(BF16)


def taps(t, low, high):
    return lambda point: t[point, low:high].reshape(-1, t.shape[-1])


def products(pieces, right, before=None):
    m = []
    for point in range(POINTS):
        left = jnp.concatenate([p[point, j] for p in pieces for j in range(PLANES)], axis=1)
        value = jnp.dot(left, right(point), preferred_element_type=F32)
        m.append(value if before is None else value + before[point])
    return m


def row_pair(m):
    return (m[1] - m[2]) - m[0], m[1] - (m[3] - m[2])


def live_phase(dims, odd, exists, multiplier, offset, bias_row, source, target, halos, s, d, t, acc, kept, emit):
    fr, cf, h, w, c = dims
    half = w // 2
    hr, hc, hk = halos
    multiplier, offset = 0.5 * multiplier, 0.5 * offset

    def act(values):
        return silu_of_half(values * multiplier + offset).astype(BF16)

    def masked(dy, dx, values):
        return jnp.where(exists(dy, dx), values.astype(F32), 0.0)

    def build_frame(f):
        def row_of(r):
            cells = act(source[f, r * w : (r + 1) * w, :])
            if f >= fr - cf:
                kept[f - (fr - cf), r * w : (r + 1) * w, :] = cells
            return cells.astype(F32)

        build(
            s.at[f],
            d.at[f],
            h,
            w,
            c,
            row_of,
            [lambda i=i: masked(SIDE[i], 0, act(hr[i, f].astype(F32))) for i in range(2)],
            [lambda i=i: masked(0, SIDE[i], act(hc[i, f].astype(F32))) for i in range(2)],
            [lambda i=i: masked(SIDE[i // 2], SIDE[i % 2], act(hk[i, f])) for i in range(4)],
        )

    zero = jnp.zeros((8, c), F32)
    sums, squares = zero, zero
    build_frame(0)
    before = None
    for o in range(fr):
        m = products([d.at[o]], taps(t, cf, cf + 1), before)
        if o + 1 < fr:
            first = max(0, o + 1 - cf)
            before = products(
                [d.at[f] for f in range(first, o + 1)], taps(t, first + cf - o - 1, cf)
            )
            build_frame(o + 1)
        both = row_pair(m)
        for q in range(2):
            y = both[q]
            if odd or o < cf:
                y = y + acc[o, q]
            else:
                y = y + jnp.concatenate([bias_row] * 2, axis=1)
            for i in range(h // 2):
                for e in range(2):
                    piece = y[i * half : (i + 1) * half, e * c : (e + 1) * c]
                    at = pl.ds((2 * i + q) * w + e, half, stride=2)
                    if odd:
                        piece = piece.astype(BF16).astype(F32)
                    target[o, at, :] = piece
                    if emit is None:
                        slabs = piece.reshape(half // 8, 8, c)
                        sums = sums + jnp.sum(slabs, axis=0)
                        squares = squares + jnp.sum(slabs * slabs, axis=0)
        if emit is not None:
            emit(o)
    return sums, squares


def kernel(dims, *refs):
    (frames, caches, weights, bias_in, gain_in, shift_in,
     mid, acc, t_last, norm, hr_last, hc_last, hk_last, kept,
     res, x, cb, wv, s, d, dc, t, small,
     s_out, s_in,
     lr_out, lc_out, lk_out, lr_in, lc_in, lk_in,
     cr_out, cc_out, ck_out, cr_in, cc_in, ck_in,
     load_sem, weight_sem, small_sem,
     stat_send, stat_recv, halo_send, halo_recv) = refs
    nh, nw, fr, cf, convs, h, w, c = dims
    peers = nh * nw
    cell_count = fr * h * w * peers * (c // GROUPS)
    clip, ha, wa = lax.axis_index("clip"), lax.axis_index("ha"), lax.axis_index("wa")
    offsets = [(i, j) for i in range(nh) for j in range(nw) if (i, j) != (0, 0)]
    others = [(lax.rem(ha + i, nh), lax.rem(wa + j, nw)) for i, j in offsets]
    exists = exists_at(nh, nw)
    barrier = pltpu.get_barrier_semaphore()
    for ph, pw in others:
        pl.semaphore_signal(barrier, inc=1, device_id=(clip, ph, pw), device_id_type=MESH)

    load_x = pltpu.make_async_copy(frames, x, load_sem.at[0])
    load_x.start()

    def span(k):
        return pl.ds(0, 1) if k == 0 else pl.ds(1, convs - 1)

    def load_cache(k):
        return pltpu.make_async_copy(caches.at[:, span(k)], cb.at[:, span(k)], load_sem.at[1 + k])

    def load_weights(k):
        return pltpu.make_async_copy(weights.at[span(k)], wv.at[span(k)], weight_sem.at[k])

    small_copies = [
        pltpu.make_async_copy(ref, small.at[i], small_sem.at[0])
        for i, ref in enumerate((bias_in, gain_in, shift_in))
    ]
    for copy in small_copies:
        copy.start()
    for k in range(2):
        load_cache(k).start()
        load_weights(k).start()
    bias, gain, shift = small.at[0], small.at[1], small.at[2]

    def halo_copy(live, k, dy, dx, towards):
        inbox = (1, 3)[k % 2] if live else (0, 2)[k]
        outbox = int(live)
        group = span(k)
        rows_out, rows_in = (lr_out, lr_in) if live else (cr_out, cr_in)
        cols_out, cols_in = (lc_out, lc_in) if live else (cc_out, cc_in)
        ends_out, ends_in = (lk_out, lk_in) if live else (ck_out, ck_in)
        if dx == 0:
            src, dst = rows_out, rows_in
            near, far = int(dy > 0), int(dy < 0)
        elif dy == 0:
            src, dst = cols_out, cols_in
            near, far = int(dx > 0), int(dx < 0)
        else:
            src, dst = ends_out, ends_in
            near = int(dy > 0) * 2 + int(dx > 0)
            far = 3 - near
        if live:
            src, dst = src.at[k, near], dst.at[k, far]
        else:
            src, dst = src.at[near, group], dst.at[far, group]
        direction = DIRECTIONS.index((dy, dx))
        back = DIRECTIONS.index((-dy, -dx))
        return pltpu.make_async_remote_copy(
            src_ref=src,
            dst_ref=dst,
            send_sem=halo_send.at[outbox, direction],
            recv_sem=halo_recv.at[inbox, back],
            device_id=(clip, ha + dy * towards, wa + dx * towards),
            device_id_type=MESH,
        )

    def pack_edges(k, field):
        for f in range(fr):
            for side in range(2):
                first = side * (w - 1)
                top = side * (h - 1) * w
                lr_out[k, side, f] = field[f, top : top + w, :].astype(BF16)
                lc_out[k, side, f] = field[f, pl.ds(first, h, stride=w), :].astype(BF16)
                for low in range(2):
                    row = low * (h - 1) * w + first
                    lk_out[k, low * 2 + side, f] = field[f, row : row + 1, :]

    def send_halo(live, k):
        for dy, dx in DIRECTIONS:

            @pl.when(exists(dy, dx))
            def _():
                halo_copy(live, k, dy, dx, 1).start()

    def wait_halo(live, k):
        for dy, dx in DIRECTIONS:

            @pl.when(exists(dy, dx))
            def _():
                halo_copy(live, k, -dy, -dx, -1).wait_recv()

    def wait_sent(live, k):
        for dy, dx in DIRECTIONS:

            @pl.when(exists(dy, dx))
            def _():
                halo_copy(live, k, dy, dx, 1).wait_send()

    def send_stats(k, sums, squares):
        s_out[k] = jnp.concatenate(
            [jnp.sum(sums, axis=0, keepdims=True), jnp.sum(squares, axis=0, keepdims=True)], axis=0
        )
        for number, (ph, pw) in enumerate(others):
            pltpu.make_async_remote_copy(
                src_ref=s_out.at[k],
                dst_ref=s_in.at[k, number],
                send_sem=stat_send.at[0],
                recv_sem=stat_recv.at[k % 2],
                device_id=(clip, ph, pw),
                device_id_type=MESH,
            ).start()

    def all_stats(k, sem):
        return pltpu.make_async_copy(s_in.at[k], s_in.at[k], sem)

    def wait_stats(k):
        all_stats(k, stat_recv.at[k % 2]).wait()
        parts = [s_out[k]] + [s_in[k, i] for i in range(peers - 1)]
        while len(parts) > 1:
            parts = [
                parts[i] + parts[i + 1] if i + 1 < len(parts) else parts[i]
                for i in range(0, len(parts), 2)
            ]
        total = jnp.concatenate([parts[0], jnp.zeros((6, c), F32)], axis=0)
        lane = lax.broadcasted_iota(jnp.int32, (8, c), 1)
        step = 1
        while step < c // GROUPS:
            total = total + jnp.where(
                lax.rem(lane, 2 * step) < step,
                pltpu.roll(total, c - step, 1),
                pltpu.roll(total, step, 1),
            )
            step *= 2
        mean = total[0:1] / cell_count
        variance = total[1:2] / cell_count - mean * mean
        multiplier = lax.rsqrt(variance + EPSILON) * gain[k : k + 1, :]
        offset = shift[k : k + 1, :] - mean * multiplier
        return multiplier, offset

    def table(k):
        return t_last if k == convs - 1 else t.at[k % 2]

    def transform_weights(k):
        if k < 2:
            load_weights(k).wait()
        into = table(k)

        def body(dt, carry):
            for dw in range(3):
                rows = slice(dw * c, (dw + 1) * c)
                g = [wv[k, dt, dh, rows, :] for dh in range(3)]
                outer = g[0].astype(F32) + g[2].astype(F32)
                inner = g[1].astype(F32)
                values = (
                    g[0],
                    (0.5 * (outer + inner)).astype(BF16),
                    (0.5 * (outer - inner)).astype(BF16),
                    g[2],
                )
                for point in range(POINTS):
                    for e in range(2):
                        j = dw + e
                        into[point, dt, j * c : (j + 1) * c, e * c : (e + 1) * c] = values[point]
            for point in range(POINTS):
                into[point, dt, 3 * c : 4 * c, 0:c] = jnp.zeros((c, c), BF16)
                into[point, dt, 0:c, c : 2 * c] = jnp.zeros((c, c), BF16)
            return carry

        lax.fori_loop(0, 3, body, 0)

    def masked(dy, dx, values):
        return jnp.where(exists(dy, dx), values, 0.0)

    def cached_phase(k):
        for f in range(cf):
            build(
                s.at[f],
                dc.at[f],
                h,
                w,
                c,
                lambda r: cb[f, k, r * w : (r + 1) * w, :].astype(F32),
                [lambda i=i: masked(SIDE[i], 0, cr_in[i, k, f].astype(F32)) for i in range(2)],
                [lambda i=i: masked(0, SIDE[i], cc_in[i, k, f].astype(F32)) for i in range(2)],
                [lambda i=i: masked(SIDE[i // 2], SIDE[i % 2], ck_in[i, k, f]) for i in range(4)],
            )
        into = table(k)
        row = bias[k : k + 1, :]
        half = w // 2
        for o in range(fr if k % 2 else cf):
            if o < cf:
                both = row_pair(products([dc.at[p] for p in range(o, cf)], taps(into, 0, cf - o)))
            for q in range(2):
                for i in range(h // 2):
                    for e in range(2):
                        rows, lanes = slice(i * half, (i + 1) * half), slice(e * c, (e + 1) * c)
                        piece = row
                        if o < cf:
                            piece = piece + both[q][rows, lanes]
                        if k % 2:
                            at = pl.ds((2 * i + q) * w + e, half, stride=2)
                            piece = piece + res[o, at, :]
                        acc[o, q, rows, lanes] = piece

    def pack_cached(k):
        if k < 2:
            load_cache(k).wait()

        for f in range(cf):
            for side in range(2):
                top = side * (h - 1) * w
                cr_out[side, k, f] = cb[f, k, top : top + w, :]
                s[f, 0 : h * w, :] = cb[f, k].astype(F32)
                first = side * (w - 1)
                cc_out[side, k, f] = s[f, pl.ds(first, h, stride=w), :].astype(BF16)
                for low in range(2):
                    row = low * (h - 1) * w + first
                    ck_out[low * 2 + side, k, f] = s[f, row : row + 1, :]

    def settle(k):
        wait_sent(True, k)
        all_stats(k, stat_send.at[0]).wait()

    load_x.wait()

    def widen(f, carry):
        sums, squares = carry
        values = x[f].astype(F32)
        res[f] = values
        slabs = values.reshape(h * w // 8, 8, c)
        return sums + jnp.sum(slabs, axis=0), squares + jnp.sum(slabs * slabs, axis=0)

    zero = jnp.zeros((8, c), F32)
    carry = lax.fori_loop(0, fr, widen, (zero, zero))
    pack_edges(0, res)
    pack_cached(0)
    pl.semaphore_wait(barrier, peers - 1)
    send_stats(0, *carry)
    send_halo(False, 0)
    transform_weights(0)
    send_halo(True, 0)
    for k in range(1, convs):
        pack_cached(k)
    pltpu.make_async_copy(small, small, small_sem.at[0]).wait()
    wait_halo(False, 0)
    cached_phase(0)
    last = convs - 1
    for k in range(convs):
        multiplier, offset = wait_stats(k)
        wait_halo(True, k)
        if k == last:
            break
        if k == 0:
            wait_sent(False, 0)
            send_halo(False, 1)
        source, target = (mid, res) if k % 2 else (res, mid)
        carry = live_phase(
            (fr, cf, h, w, c), k % 2, exists, multiplier, offset, bias[k : k + 1, :],
            source, target, (lr_in.at[k], lc_in.at[k], lk_in.at[k]),
            s, d, table(k), acc, kept.at[k], None,
        )
        settle(k)
        send_stats(k + 1, *carry)
        pack_edges(k + 1, target)
        send_halo(True, k + 1)
        transform_weights(k + 1)
        if k == 0:
            wait_halo(False, 1)
        cached_phase(k + 1)
        if k == 0:
            wait_sent(False, 1)

    norm[...] = jnp.zeros_like(norm)
    norm[0:1] = multiplier
    norm[1:2] = offset
    norm[2:3] = bias[last : last + 1, :]
    hr_last[...] = lr_in[last]
    hc_last[...] = lc_in[last]
    hk_last[...] = lk_in[last]
    settle(last)


def finish(dims, *refs):
    (mid, acc, t_last, norm_last, hr, hc, hk, kept,
     encoded, new_caches,
     s, d, out, kept_new, y, out_sem, kept_sem) = refs
    nh, nw, fr, cf, convs, h, w, c = dims
    exists = exists_at(nh, nw)
    copies = [
        pltpu.make_async_copy(kept.at[k], new_caches.at[:, k], kept_sem.at[k])
        for k in range(convs - 1)
    ]
    for copy in copies:
        copy.start()

    def emit(o):
        out[o] = y[o].astype(BF16)

    live_phase(
        (fr, cf, h, w, c), (convs - 1) % 2, exists, norm_last[0:1], norm_last[1:2], norm_last[2:3],
        mid, y, (hr, hc, hk), s, d, t_last, acc, kept_new, emit,
    )
    copies.append(
        pltpu.make_async_copy(kept_new, new_caches.at[:, convs - 1], kept_sem.at[convs - 1])
    )
    copies[-1].start()
    copies.append(pltpu.make_async_copy(out, encoded, out_sem.at[0]))
    copies[-1].start()
    for copy in copies:
        copy.wait()


def local(nh, nw, frames, caches, conv_weights, conv_bias, norm_gain, norm_shift):
    fr, h, w, c = frames.shape
    cf, convs = caches.shape[:2]
    dims = (nh, nw, fr, cf, convs, h, w, c)
    peers = nh * nw
    vmem = pltpu.VMEM
    dma = pltpu.SemaphoreType.DMA
    pitch = w + 2 * LEAD
    pairs = h * w // 4
    s_shape = vmem((fr, (h + 2) * pitch, c), F32)
    d_shape = vmem((fr, POINTS, PLANES, pairs, c), BF16)
    table = (POINTS, cf + 1, PLANES * c, 2 * c)
    scratch = [
        vmem((fr, h * w, c), F32),
        vmem((fr, h * w, c), BF16),
        vmem((cf, convs, h * w, c), BF16),
        vmem((convs, 3, 3, 3 * c, c), BF16),
        s_shape,
        d_shape,
        vmem((cf, POINTS, PLANES, pairs, c), BF16),
        vmem((2,) + table, BF16),
        vmem((3, convs, c), F32),
        vmem((convs, 2, c), F32),
        vmem((convs, peers - 1, 2, c), F32),
    ]
    for _ in range(2):
        scratch += [
            vmem((convs, 2, fr, w, c), BF16),
            vmem((convs, 2, fr, h, c), BF16),
            vmem((convs, 4, fr, 1, c), F32),
        ]
    for _ in range(2):
        scratch += [
            vmem((2, convs, cf, w, c), BF16),
            vmem((2, convs, cf, h, c), BF16),
            vmem((4, convs, cf, 1, c), F32),
        ]
    scratch += [
        dma((3,)),
        dma((2,)),
        dma((1,)),
        dma((1,)),
        dma((2,)),
        dma((2, 8)),
        dma((4, 8)),
    ]
    anywhere = pl.BlockSpec(memory_space=pltpu.HBM)
    inside = pl.BlockSpec(memory_space=pltpu.VMEM)
    handed = [
        ((fr, h * w, c), F32),
        ((fr, 2, pairs, 2 * c), F32),
        (table, BF16),
        ((8, c), F32),
        ((2, fr, w, c), BF16),
        ((2, fr, h, c), BF16),
        ((4, fr, 1, c), F32),
        ((convs - 1, cf, h * w, c), BF16),
    ]
    state = pl.pallas_call(
        functools.partial(kernel, dims),
        out_shape=[vmem(shape, dtype) for shape, dtype in handed],
        in_specs=[anywhere] * 6,
        out_specs=[inside] * len(handed),
        scratch_shapes=scratch,
        compiler_params=pltpu.CompilerParams(
            collective_id=0, has_side_effects=True, vmem_limit_bytes=48 * 1024 * 1024
        ),
    )(
        frames.reshape(fr, h * w, c),
        caches.reshape(cf, convs, h * w, c),
        conv_weights.reshape(convs, 3, 3, 3 * c, c),
        conv_bias,
        norm_gain,
        norm_shift,
    )
    encoded, new_caches = pl.pallas_call(
        functools.partial(finish, dims),
        out_shape=(
            jax.ShapeDtypeStruct((fr, h * w, c), BF16),
            jax.ShapeDtypeStruct((cf, convs, h * w, c), BF16),
        ),
        in_specs=[inside] * len(handed),
        out_specs=(anywhere, anywhere),
        scratch_shapes=[
            s_shape,
            d_shape,
            vmem((fr, h * w, c), BF16),
            vmem((cf, h * w, c), BF16),
            vmem((fr, h * w, c), F32),
            dma((1,)),
            dma((convs,)),
        ],
        compiler_params=pltpu.CompilerParams(vmem_limit_bytes=24 * 1024 * 1024),
    )(*state)
    return encoded.reshape(frames.shape), new_caches.reshape(caches.shape)


def solution(mesh):
    return jax.shard_map(
        functools.partial(local, mesh.shape["ha"], mesh.shape["wa"]),
        mesh=mesh,
        in_specs=(
            P("clip", "ha", "wa", None),
            P("clip", None, "ha", "wa", None),
            P(),
            P(),
            P(),
            P(),
        ),
        out_specs=(P("clip", "ha", "wa", None), P("clip", None, "ha", "wa", None)),
        check_vma=False,
    )
```

```python
import functools

import jax
import jax.numpy as jnp
from jax import lax
from jax.experimental import pallas as pl
from jax.experimental.pallas import tpu as pltpu
from jax.sharding import PartitionSpec as P

GROUPS = 32
EPSILON = 1e-06
MESH = pl.DeviceIdType.MESH
F32 = jnp.float32
BF16 = jnp.bfloat16
DIRECTIONS = [(dy, dx) for dy in (-1, 0, 1) for dx in (-1, 0, 1) if (dy, dx) != (0, 0)]
SIDE = (-1, 1)
LEAD = 8
POINTS = 4
PLANES = 4


def silu_of_half(half):
    return half + half * jnp.tanh(half)


def exists_at(nh, nw):
    ha, wa = lax.axis_index("ha"), lax.axis_index("wa")

    def exists(dy, dx):
        conds = []
        if dy:
            conds.append(ha > 0 if dy < 0 else ha < nh - 1)
        if dx:
            conds.append(wa > 0 if dx < 0 else wa < nw - 1)
        return conds[0] if len(conds) == 1 else jnp.logical_and(*conds)

    return exists


def build(s, d, h, w, c, row_of, rows, cols, ends):
    pitch = w + 2 * LEAD
    half = w // 2
    for r in range(h + 2):
        cells = rows[0]() if r == 0 else rows[1]() if r == h + 1 else row_of(r - 1)
        at = r * pitch + LEAD
        s[at : at + w, :] = cells
    for side in range(2):
        edge = LEAD - 1 + side * (w + 1)
        s[pl.ds(pitch + edge, h, stride=pitch), :] = cols[side]()
        for low in range(2):
            at = low * (h + 1) * pitch + edge
            s[at : at + 1, :] = ends[low * 2 + side]()

    def planes(r):
        return [
            s[pl.ds(r * pitch + LEAD - 1 + j, half, stride=2), :] for j in range(PLANES)
        ]

    window = [planes(0), planes(1)]
    for i in range(h // 2):
        window = window[-2:] + [planes(2 * i + 2), planes(2 * i + 3)]
        for j in range(PLANES):
            r0, r1, r2, r3 = (row[j] for row in window)
            for point, value in enumerate((r2 - r0, r1 + r2, r1 - r2, r1 - r3)):
                d[point, j, i * half : (i + 1) * half, :] = value.astype(BF16)


def taps(t, low, high):
    return lambda point: t[point, low:high].reshape(-1, t.shape[-1])


def products(pieces, right, before=None):
    m = []
    for point in range(POINTS):
        left = jnp.concatenate([p[point, j] for p in pieces for j in range(PLANES)], axis=1)
        value = jnp.dot(left, right(point), preferred_element_type=F32)
        m.append(value if before is None else value + before[point])
    return m


def row_pair(m):
    return (m[1] - m[2]) - m[0], m[1] - (m[3] - m[2])


def live_phase(dims, odd, exists, multiplier, offset, bias_row, source, target, halos, s, d, t, acc, kept, emit):
    fr, cf, h, w, c = dims
    half = w // 2
    hr, hc, hk = halos
    multiplier, offset = 0.5 * multiplier, 0.5 * offset

    def act(values):
        return silu_of_half(values * multiplier + offset).astype(BF16)

    def masked(dy, dx, values):
        return jnp.where(exists(dy, dx), values.astype(F32), 0.0)

    def build_frame(f):
        def row_of(r):
            cells = act(source[f, r * w : (r + 1) * w, :])
            if f >= fr - cf:
                kept[f - (fr - cf), r * w : (r + 1) * w, :] = cells
            return cells.astype(F32)

        build(
            s.at[f],
            d.at[f],
            h,
            w,
            c,
            row_of,
            [lambda i=i: masked(SIDE[i], 0, act(hr[i, f].astype(F32))) for i in range(2)],
            [lambda i=i: masked(0, SIDE[i], act(hc[i, f].astype(F32))) for i in range(2)],
            [lambda i=i: masked(SIDE[i // 2], SIDE[i % 2], act(hk[i, f])) for i in range(4)],
        )

    zero = jnp.zeros((8, c), F32)
    sums, squares = zero, zero
    build_frame(0)
    before = None
    for o in range(fr):
        m = products([d.at[o]], taps(t, cf, cf + 1), before)
        if o + 1 < fr:
            first = max(0, o + 1 - cf)
            before = products(
                [d.at[f] for f in range(first, o + 1)], taps(t, first + cf - o - 1, cf)
            )
            build_frame(o + 1)
        both = row_pair(m)
        for q in range(2):
            y = both[q]
            if odd or o < cf:
                y = y + acc[o, q]
            else:
                y = y + jnp.concatenate([bias_row] * 2, axis=1)
            for i in range(h // 2):
                for e in range(2):
                    piece = y[i * half : (i + 1) * half, e * c : (e + 1) * c]
                    at = pl.ds((2 * i + q) * w + e, half, stride=2)
                    if odd:
                        piece = piece.astype(BF16).astype(F32)
                    target[o, at, :] = piece
                    if emit is None:
                        slabs = piece.reshape(half // 8, 8, c)
                        sums = sums + jnp.sum(slabs, axis=0)
                        squares = squares + jnp.sum(slabs * slabs, axis=0)
        if emit is not None:
            emit(o)
    return sums, squares


def kernel(dims, *refs):
    (frames, caches, weights, bias_in, gain_in, shift_in,
     mid, acc, t_last, norm, hr_last, hc_last, hk_last, kept,
     res, x, cb, wv, s, d, dc, t, small,
     s_out, s_in,
     lr_out, lc_out, lk_out, lr_in, lc_in, lk_in,
     cr_out, cc_out, ck_out, cr_in, cc_in, ck_in,
     load_sem, weight_sem, small_sem,
     stat_send, stat_recv, halo_send, halo_recv) = refs
    nh, nw, fr, cf, convs, h, w, c = dims
    peers = nh * nw
    cell_count = fr * h * w * peers * (c // GROUPS)
    clip, ha, wa = lax.axis_index("clip"), lax.axis_index("ha"), lax.axis_index("wa")
    offsets = sorted(
        ((i, j) for i in range(nh) for j in range(nw) if (i, j) != (0, 0)),
        key=lambda ij: -sum((x % 2) * 2 + (x > 0) for x in ij),
    )
    others = [(lax.rem(ha + i, nh), lax.rem(wa + j, nw)) for i, j in offsets]
    exists = exists_at(nh, nw)
    barrier = pltpu.get_barrier_semaphore()
    for ph, pw in others:
        pl.semaphore_signal(barrier, inc=1, device_id=(clip, ph, pw), device_id_type=MESH)

    load_x = pltpu.make_async_copy(frames, x, load_sem.at[0])
    load_x.start()

    def span(k):
        return pl.ds(0, 1) if k == 0 else pl.ds(1, convs - 1)

    def load_cache(k):
        return pltpu.make_async_copy(caches.at[:, span(k)], cb.at[:, span(k)], load_sem.at[1 + k])

    def load_weights(k):
        return pltpu.make_async_copy(weights.at[span(k)], wv.at[span(k)], weight_sem.at[k])

    small_copies = [
        pltpu.make_async_copy(ref, small.at[i], small_sem.at[0])
        for i, ref in enumerate((bias_in, gain_in, shift_in))
    ]
    for copy in small_copies:
        copy.start()
    for k in range(2):
        load_cache(k).start()
        load_weights(k).start()
    bias, gain, shift = small.at[0], small.at[1], small.at[2]

    def halo_copy(live, k, dy, dx, towards):
        inbox = (1, 3)[k % 2] if live else (0, 2)[k]
        outbox = int(live)
        group = span(k)
        rows_out, rows_in = (lr_out, lr_in) if live else (cr_out, cr_in)
        cols_out, cols_in = (lc_out, lc_in) if live else (cc_out, cc_in)
        ends_out, ends_in = (lk_out, lk_in) if live else (ck_out, ck_in)
        if dx == 0:
            src, dst = rows_out, rows_in
            near, far = int(dy > 0), int(dy < 0)
        elif dy == 0:
            src, dst = cols_out, cols_in
            near, far = int(dx > 0), int(dx < 0)
        else:
            src, dst = ends_out, ends_in
            near = int(dy > 0) * 2 + int(dx > 0)
            far = 3 - near
        if live:
            src, dst = src.at[k, near], dst.at[k, far]
        else:
            src, dst = src.at[near, group], dst.at[far, group]
        direction = DIRECTIONS.index((dy, dx))
        back = DIRECTIONS.index((-dy, -dx))
        return pltpu.make_async_remote_copy(
            src_ref=src,
            dst_ref=dst,
            send_sem=halo_send.at[outbox, direction],
            recv_sem=halo_recv.at[inbox, back],
            device_id=(clip, ha + dy * towards, wa + dx * towards),
            device_id_type=MESH,
        )

    def pack_edges(k, field):
        for f in range(fr):
            for side in range(2):
                first = side * (w - 1)
                top = side * (h - 1) * w
                lr_out[k, side, f] = field[f, top : top + w, :].astype(BF16)
                lc_out[k, side, f] = field[f, pl.ds(first, h, stride=w), :].astype(BF16)
                for low in range(2):
                    row = low * (h - 1) * w + first
                    lk_out[k, low * 2 + side, f] = field[f, row : row + 1, :]

    def send_halo(live, k):
        for dy, dx in DIRECTIONS:

            @pl.when(exists(dy, dx))
            def _():
                halo_copy(live, k, dy, dx, 1).start()

    def wait_halo(live, k):
        for dy, dx in DIRECTIONS:

            @pl.when(exists(dy, dx))
            def _():
                halo_copy(live, k, -dy, -dx, -1).wait_recv()

    def wait_sent(live, k):
        for dy, dx in DIRECTIONS:

            @pl.when(exists(dy, dx))
            def _():
                halo_copy(live, k, dy, dx, 1).wait_send()

    def send_stats(k, sums, squares):
        s_out[k] = jnp.concatenate(
            [jnp.sum(sums, axis=0, keepdims=True), jnp.sum(squares, axis=0, keepdims=True)], axis=0
        )
        for number, (ph, pw) in enumerate(others):
            pltpu.make_async_remote_copy(
                src_ref=s_out.at[k],
                dst_ref=s_in.at[k, number],
                send_sem=stat_send.at[0],
                recv_sem=stat_recv.at[k % 2],
                device_id=(clip, ph, pw),
                device_id_type=MESH,
            ).start()

    def all_stats(k, sem):
        return pltpu.make_async_copy(s_in.at[k], s_in.at[k], sem)

    def wait_stats(k):
        all_stats(k, stat_recv.at[k % 2]).wait()
        parts = [s_out[k]] + [s_in[k, i] for i in range(peers - 1)]
        while len(parts) > 1:
            parts = [
                parts[i] + parts[i + 1] if i + 1 < len(parts) else parts[i]
                for i in range(0, len(parts), 2)
            ]
        rows = jnp.concatenate([parts[0], jnp.zeros((6, c), F32)], axis=0)
        size = c // GROUPS
        place = lax.rem(lax.broadcasted_iota(jnp.int32, (8, c), 1), size)
        total = rows
        for step in range(1, size):
            total = total + jnp.where(place + step < size, pltpu.roll(rows, c - step, 1), 0.0)
            total = total + jnp.where(place >= step, pltpu.roll(rows, step, 1), 0.0)
        mean = total[0:1] / cell_count
        variance = total[1:2] / cell_count - mean * mean
        multiplier = lax.rsqrt(variance + EPSILON) * gain[k : k + 1, :]
        offset = shift[k : k + 1, :] - mean * multiplier
        return multiplier, offset

    def table(k):
        return t_last if k == convs - 1 else t.at[k % 2]

    def transform_weights(k):
        if k < 2:
            load_weights(k).wait()
        into = table(k)

        def body(dt, carry):
            for dw in range(3):
                rows = slice(dw * c, (dw + 1) * c)
                g = [wv[k, dt, dh, rows, :] for dh in range(3)]
                outer = g[0].astype(F32) + g[2].astype(F32)
                inner = g[1].astype(F32)
                values = (
                    g[0],
                    (0.5 * (outer + inner)).astype(BF16),
                    (0.5 * (outer - inner)).astype(BF16),
                    g[2],
                )
                for point in range(POINTS):
                    for e in range(2):
                        j = dw + e
                        into[point, dt, j * c : (j + 1) * c, e * c : (e + 1) * c] = values[point]
            for point in range(POINTS):
                into[point, dt, 3 * c : 4 * c, 0:c] = jnp.zeros((c, c), BF16)
                into[point, dt, 0:c, c : 2 * c] = jnp.zeros((c, c), BF16)
            return carry

        lax.fori_loop(0, 3, body, 0)

    def masked(dy, dx, values):
        return jnp.where(exists(dy, dx), values, 0.0)

    def cached_phase(k):
        for f in range(cf):
            build(
                s.at[f],
                dc.at[f],
                h,
                w,
                c,
                lambda r: cb[f, k, r * w : (r + 1) * w, :].astype(F32),
                [lambda i=i: masked(SIDE[i], 0, cr_in[i, k, f].astype(F32)) for i in range(2)],
                [lambda i=i: masked(0, SIDE[i], cc_in[i, k, f].astype(F32)) for i in range(2)],
                [lambda i=i: masked(SIDE[i // 2], SIDE[i % 2], ck_in[i, k, f]) for i in range(4)],
            )
        into = table(k)
        row = bias[k : k + 1, :]
        half = w // 2
        for o in range(fr if k % 2 else cf):
            if o < cf:
                both = row_pair(products([dc.at[p] for p in range(o, cf)], taps(into, 0, cf - o)))
            for q in range(2):
                for i in range(h // 2):
                    for e in range(2):
                        rows, lanes = slice(i * half, (i + 1) * half), slice(e * c, (e + 1) * c)
                        piece = row
                        if o < cf:
                            piece = piece + both[q][rows, lanes]
                        if k % 2:
                            at = pl.ds((2 * i + q) * w + e, half, stride=2)
                            piece = piece + res[o, at, :]
                        acc[o, q, rows, lanes] = piece

    def pack_cached(k):
        if k < 2:
            load_cache(k).wait()

        for f in range(cf):
            for side in range(2):
                top = side * (h - 1) * w
                cr_out[side, k, f] = cb[f, k, top : top + w, :]
                s[f, 0 : h * w, :] = cb[f, k].astype(F32)
                first = side * (w - 1)
                cc_out[side, k, f] = s[f, pl.ds(first, h, stride=w), :].astype(BF16)
                for low in range(2):
                    row = low * (h - 1) * w + first
                    ck_out[low * 2 + side, k, f] = s[f, row : row + 1, :]

    def settle(k):
        wait_sent(True, k)
        all_stats(k, stat_send.at[0]).wait()

    load_x.wait()

    def widen(f, carry):
        sums, squares = carry
        values = x[f].astype(F32)
        res[f] = values
        slabs = values.reshape(h * w // 8, 8, c)
        return sums + jnp.sum(slabs, axis=0), squares + jnp.sum(slabs * slabs, axis=0)

    zero = jnp.zeros((8, c), F32)
    carry = lax.fori_loop(0, fr, widen, (zero, zero))
    pack_edges(0, res)
    pack_cached(0)
    pl.semaphore_wait(barrier, peers - 1)
    send_stats(0, *carry)
    send_halo(False, 0)
    transform_weights(0)
    send_halo(True, 0)
    for k in range(1, convs):
        pack_cached(k)
    pltpu.make_async_copy(small, small, small_sem.at[0]).wait()
    wait_halo(False, 0)
    cached_phase(0)
    wait_sent(False, 0)
    last = convs - 1
    settle(0)
    for k in range(convs):
        multiplier, offset = wait_stats(k)
        wait_halo(True, k)
        if k == last:
            break
        if k == 0:
            send_halo(False, 1)
        source, target = (mid, res) if k % 2 else (res, mid)
        carry = live_phase(
            (fr, cf, h, w, c), k % 2, exists, multiplier, offset, bias[k : k + 1, :],
            source, target, (lr_in.at[k], lc_in.at[k], lk_in.at[k]),
            s, d, table(k), acc, kept.at[k], None,
        )
        send_stats(k + 1, *carry)
        pack_edges(k + 1, target)
        send_halo(True, k + 1)
        transform_weights(k + 1)
        if k == 0:
            wait_halo(False, 1)
        cached_phase(k + 1)
        if k == 0:
            wait_sent(False, 1)
        settle(k + 1)

    norm[...] = jnp.zeros_like(norm)
    norm[0:1] = multiplier
    norm[1:2] = offset
    norm[2:3] = bias[last : last + 1, :]
    hr_last[...] = lr_in[last]
    hc_last[...] = lc_in[last]
    hk_last[...] = lk_in[last]


def finish(dims, *refs):
    (mid, acc, t_last, norm_last, hr, hc, hk, kept,
     encoded, new_caches,
     s, d, out, kept_new, y, out_sem, kept_sem) = refs
    nh, nw, fr, cf, convs, h, w, c = dims
    exists = exists_at(nh, nw)
    copies = [
        pltpu.make_async_copy(kept.at[k], new_caches.at[:, k], kept_sem.at[k])
        for k in range(convs - 1)
    ]
    for copy in copies:
        copy.start()

    def emit(o):
        out[o] = y[o].astype(BF16)

    live_phase(
        (fr, cf, h, w, c), (convs - 1) % 2, exists, norm_last[0:1], norm_last[1:2], norm_last[2:3],
        mid, y, (hr, hc, hk), s, d, t_last, acc, kept_new, emit,
    )
    copies.append(
        pltpu.make_async_copy(kept_new, new_caches.at[:, convs - 1], kept_sem.at[convs - 1])
    )
    copies[-1].start()
    copies.append(pltpu.make_async_copy(out, encoded, out_sem.at[0]))
    copies[-1].start()
    for copy in copies:
        copy.wait()


def local(nh, nw, frames, caches, conv_weights, conv_bias, norm_gain, norm_shift):
    fr, h, w, c = frames.shape
    cf, convs = caches.shape[:2]
    dims = (nh, nw, fr, cf, convs, h, w, c)
    peers = nh * nw
    vmem = pltpu.VMEM
    dma = pltpu.SemaphoreType.DMA
    pitch = w + 2 * LEAD
    pairs = h * w // 4
    s_shape = vmem((fr, (h + 2) * pitch, c), F32)
    d_shape = vmem((fr, POINTS, PLANES, pairs, c), BF16)
    table = (POINTS, cf + 1, PLANES * c, 2 * c)
    scratch = [
        vmem((fr, h * w, c), F32),
        vmem((fr, h * w, c), BF16),
        vmem((cf, convs, h * w, c), BF16),
        vmem((convs, 3, 3, 3 * c, c), BF16),
        s_shape,
        d_shape,
        vmem((cf, POINTS, PLANES, pairs, c), BF16),
        vmem((2,) + table, BF16),
        vmem((3, convs, c), F32),
        vmem((convs, 2, c), F32),
        vmem((convs, peers - 1, 2, c), F32),
    ]
    for _ in range(2):
        scratch += [
            vmem((convs, 2, fr, w, c), BF16),
            vmem((convs, 2, fr, h, c), BF16),
            vmem((convs, 4, fr, 1, c), F32),
        ]
    for _ in range(2):
        scratch += [
            vmem((2, convs, cf, w, c), BF16),
            vmem((2, convs, cf, h, c), BF16),
            vmem((4, convs, cf, 1, c), F32),
        ]
    scratch += [
        dma((3,)),
        dma((2,)),
        dma((1,)),
        dma((1,)),
        dma((2,)),
        dma((2, 8)),
        dma((4, 8)),
    ]
    anywhere = pl.BlockSpec(memory_space=pltpu.HBM)
    inside = pl.BlockSpec(memory_space=pltpu.VMEM)
    handed = [
        ((fr, h * w, c), F32),
        ((fr, 2, pairs, 2 * c), F32),
        (table, BF16),
        ((8, c), F32),
        ((2, fr, w, c), BF16),
        ((2, fr, h, c), BF16),
        ((4, fr, 1, c), F32),
        ((convs - 1, cf, h * w, c), BF16),
    ]
    state = pl.pallas_call(
        functools.partial(kernel, dims),
        out_shape=[vmem(shape, dtype) for shape, dtype in handed],
        in_specs=[anywhere] * 6,
        out_specs=[inside] * len(handed),
        scratch_shapes=scratch,
        compiler_params=pltpu.CompilerParams(
            collective_id=0, has_side_effects=True, vmem_limit_bytes=48 * 1024 * 1024
        ),
    )(
        frames.reshape(fr, h * w, c),
        caches.reshape(cf, convs, h * w, c),
        conv_weights.reshape(convs, 3, 3, 3 * c, c),
        conv_bias,
        norm_gain,
        norm_shift,
    )
    encoded, new_caches = pl.pallas_call(
        functools.partial(finish, dims),
        out_shape=(
            jax.ShapeDtypeStruct((fr, h * w, c), BF16),
            jax.ShapeDtypeStruct((cf, convs, h * w, c), BF16),
        ),
        in_specs=[inside] * len(handed),
        out_specs=(anywhere, anywhere),
        scratch_shapes=[
            s_shape,
            d_shape,
            vmem((fr, h * w, c), BF16),
            vmem((cf, h * w, c), BF16),
            vmem((fr, h * w, c), F32),
            dma((1,)),
            dma((convs,)),
        ],
        compiler_params=pltpu.CompilerParams(vmem_limit_bytes=24 * 1024 * 1024),
    )(*state)
    return encoded.reshape(frames.shape), new_caches.reshape(caches.shape)


def solution(mesh):
    return jax.shard_map(
        functools.partial(local, mesh.shape["ha"], mesh.shape["wa"]),
        mesh=mesh,
        in_specs=(
            P("clip", "ha", "wa", None),
            P("clip", None, "ha", "wa", None),
            P(),
            P(),
            P(),
            P(),
        ),
        out_specs=(P("clip", "ha", "wa", None), P("clip", None, "ha", "wa", None)),
        check_vma=False,
    )
```

```python
import functools

import jax
import jax.numpy as jnp
from jax import lax
from jax.experimental import pallas as pl
from jax.experimental.pallas import tpu as pltpu
from jax.sharding import PartitionSpec as P

GROUPS = 32
EPSILON = 1e-06
MESH = pl.DeviceIdType.MESH
F32 = jnp.float32
BF16 = jnp.bfloat16
DIRECTIONS = [(dy, dx) for dy in (-1, 0, 1) for dx in (-1, 0, 1) if (dy, dx) != (0, 0)]
SIDE = (-1, 1)
LEAD = 8
POINTS = 4
PLANES = 4


def silu_of_half(half):
    return half + half * jnp.tanh(half)


def exists_at(nh, nw):
    ha, wa = lax.axis_index("ha"), lax.axis_index("wa")

    def exists(dy, dx):
        conds = []
        if dy:
            conds.append(ha > 0 if dy < 0 else ha < nh - 1)
        if dx:
            conds.append(wa > 0 if dx < 0 else wa < nw - 1)
        return conds[0] if len(conds) == 1 else jnp.logical_and(*conds)

    return exists


def build(s, d, h, w, c, row_of, rows, cols, ends):
    pitch = w + 2 * LEAD
    half = w // 2
    for r in range(h + 2):
        cells = rows[0]() if r == 0 else rows[1]() if r == h + 1 else row_of(r - 1)
        at = r * pitch + LEAD
        s[at : at + w, :] = cells
    for side in range(2):
        edge = LEAD - 1 + side * (w + 1)
        s[pl.ds(pitch + edge, h, stride=pitch), :] = cols[side]()
        for low in range(2):
            at = low * (h + 1) * pitch + edge
            s[at : at + 1, :] = ends[low * 2 + side]()

    def planes(r):
        return [
            s[pl.ds(r * pitch + LEAD - 1 + j, half, stride=2), :] for j in range(PLANES)
        ]

    window = [planes(0), planes(1)]
    for i in range(h // 2):
        window = window[-2:] + [planes(2 * i + 2), planes(2 * i + 3)]
        for j in range(PLANES):
            r0, r1, r2, r3 = (row[j] for row in window)
            for point, value in enumerate((r2 - r0, r1 + r2, r1 - r2, r1 - r3)):
                d[point, j, i * half : (i + 1) * half, :] = value.astype(BF16)


def taps(t, low, high):
    return lambda point: t[point, low:high].reshape(-1, t.shape[-1])


def products(pieces, right, before=None):
    m = []
    for point in range(POINTS):
        left = jnp.concatenate([p[point, j] for p in pieces for j in range(PLANES)], axis=1)
        value = jnp.dot(left, right(point), preferred_element_type=F32)
        m.append(value if before is None else value + before[point])
    return m


def row_pair(m):
    return (m[1] - m[2]) - m[0], m[1] - (m[3] - m[2])


def live_phase(dims, odd, exists, multiplier, offset, bias_row, source, target, halos, s, d, t, acc, kept, emit, midway=None):
    fr, cf, h, w, c = dims
    half = w // 2
    hr, hc, hk = halos
    multiplier, offset = 0.5 * multiplier, 0.5 * offset

    def act(values):
        return silu_of_half(values * multiplier + offset).astype(BF16)

    def masked(dy, dx, values):
        return jnp.where(exists(dy, dx), values.astype(F32), 0.0)

    def build_frame(f):
        def row_of(r):
            cells = act(source[f, r * w : (r + 1) * w, :])
            if f >= fr - cf:
                kept[f - (fr - cf), r * w : (r + 1) * w, :] = cells
            return cells.astype(F32)

        build(
            s.at[f],
            d.at[f],
            h,
            w,
            c,
            row_of,
            [lambda i=i: masked(SIDE[i], 0, act(hr[i, f].astype(F32))) for i in range(2)],
            [lambda i=i: masked(0, SIDE[i], act(hc[i, f].astype(F32))) for i in range(2)],
            [lambda i=i: masked(SIDE[i // 2], SIDE[i % 2], act(hk[i, f])) for i in range(4)],
        )

    zero = jnp.zeros((8, c), F32)
    sums, squares = zero, zero
    build_frame(0)
    before = None
    for o in range(fr):
        if o == fr - 1 and midway is not None:
            midway()
        m = products([d.at[o]], taps(t, cf, cf + 1), before)
        if o + 1 < fr:
            first = max(0, o + 1 - cf)
            before = products(
                [d.at[f] for f in range(first, o + 1)], taps(t, first + cf - o - 1, cf)
            )
            build_frame(o + 1)
        both = row_pair(m)
        for q in range(2):
            y = both[q]
            if odd or o < cf:
                y = y + acc[o, q]
            else:
                y = y + jnp.concatenate([bias_row] * 2, axis=1)
            for i in range(h // 2):
                for e in range(2):
                    piece = y[i * half : (i + 1) * half, e * c : (e + 1) * c]
                    at = pl.ds((2 * i + q) * w + e, half, stride=2)
                    if odd:
                        piece = piece.astype(BF16).astype(F32)
                    target[o, at, :] = piece
                    if emit is None:
                        slabs = piece.reshape(half // 8, 8, c)
                        sums = sums + jnp.sum(slabs, axis=0)
                        squares = squares + jnp.sum(slabs * slabs, axis=0)
        if emit is not None:
            emit(o)
    return sums, squares


def kernel(dims, *refs):
    (frames, caches, weights, bias_in, gain_in, shift_in,
     mid, acc, t_last, norm, hr_last, hc_last, hk_last, kept,
     res, x, cb, wv, s, d, dc, t, small,
     s_out, s_in,
     lr_out, lc_out, lk_out, lr_in, lc_in, lk_in,
     cr_out, cc_out, ck_out, cr_in, cc_in, ck_in,
     load_sem, weight_sem, small_sem,
     stat_send, stat_recv, halo_send, halo_recv) = refs
    nh, nw, fr, cf, convs, h, w, c = dims
    peers = nh * nw
    cell_count = fr * h * w * peers * (c // GROUPS)
    clip, ha, wa = lax.axis_index("clip"), lax.axis_index("ha"), lax.axis_index("wa")
    offsets = sorted(
        ((i, j) for i in range(nh) for j in range(nw) if (i, j) != (0, 0)),
        key=lambda ij: -sum((x % 2) * 2 + (x > 0) for x in ij),
    )
    others = [(lax.rem(ha + i, nh), lax.rem(wa + j, nw)) for i, j in offsets]
    exists = exists_at(nh, nw)
    barrier = pltpu.get_barrier_semaphore()
    for ph, pw in others:
        pl.semaphore_signal(barrier, inc=1, device_id=(clip, ph, pw), device_id_type=MESH)

    load_x = pltpu.make_async_copy(frames, x, load_sem.at[0])
    load_x.start()

    def span(k):
        return pl.ds(0, 1) if k == 0 else pl.ds(1, convs - 1)

    def load_cache(k):
        return pltpu.make_async_copy(caches.at[:, span(k)], cb.at[:, span(k)], load_sem.at[1 + k])

    def load_weights(k):
        return pltpu.make_async_copy(weights.at[span(k)], wv.at[span(k)], weight_sem.at[k])

    small_copies = [
        pltpu.make_async_copy(ref, small.at[i], small_sem.at[0])
        for i, ref in enumerate((bias_in, gain_in, shift_in))
    ]
    for copy in small_copies:
        copy.start()
    for k in range(2):
        load_cache(k).start()
        load_weights(k).start()
    bias, gain, shift = small.at[0], small.at[1], small.at[2]

    def halo_copy(live, k, dy, dx, towards):
        inbox = (1, 3)[k % 2] if live else (0, 2)[k]
        group = span(k)
        rows_out, rows_in = (lr_out, lr_in) if live else (cr_out, cr_in)
        cols_out, cols_in = (lc_out, lc_in) if live else (cc_out, cc_in)
        ends_out, ends_in = (lk_out, lk_in) if live else (ck_out, ck_in)
        if dx == 0:
            src, dst = rows_out, rows_in
            near, far = int(dy > 0), int(dy < 0)
        elif dy == 0:
            src, dst = cols_out, cols_in
            near, far = int(dx > 0), int(dx < 0)
        else:
            src, dst = ends_out, ends_in
            near = int(dy > 0) * 2 + int(dx > 0)
            far = 3 - near
        if live:
            src, dst = src.at[k, near], dst.at[k, far]
        else:
            src, dst = src.at[near, group], dst.at[far, group]
        direction = DIRECTIONS.index((dy, dx))
        back = DIRECTIONS.index((-dy, -dx))
        return pltpu.make_async_remote_copy(
            src_ref=src,
            dst_ref=dst,
            send_sem=halo_send.at[direction],
            recv_sem=halo_recv.at[inbox, back],
            device_id=(clip, ha + dy * towards, wa + dx * towards),
            device_id_type=MESH,
        )

    def pack_edges(k, field):
        for f in range(fr):
            for side in range(2):
                first = side * (w - 1)
                top = side * (h - 1) * w
                lr_out[k, side, f] = field[f, top : top + w, :].astype(BF16)
                lc_out[k, side, f] = field[f, pl.ds(first, h, stride=w), :].astype(BF16)
                for low in range(2):
                    row = low * (h - 1) * w + first
                    lk_out[k, low * 2 + side, f] = field[f, row : row + 1, :]

    def send_halo(live, k):
        for dy, dx in DIRECTIONS:

            @pl.when(exists(dy, dx))
            def _():
                halo_copy(live, k, dy, dx, 1).start()

    def wait_halo(live, k):
        for dy, dx in DIRECTIONS:

            @pl.when(exists(dy, dx))
            def _():
                halo_copy(live, k, -dy, -dx, -1).wait_recv()

    def wait_sent(live, k):
        for dy, dx in DIRECTIONS:

            @pl.when(exists(dy, dx))
            def _():
                halo_copy(live, k, dy, dx, 1).wait_send()

    def send_stats(k, sums, squares):
        s_out[k] = jnp.concatenate(
            [jnp.sum(sums, axis=0, keepdims=True), jnp.sum(squares, axis=0, keepdims=True)], axis=0
        )
        for number, (ph, pw) in enumerate(others):
            pltpu.make_async_remote_copy(
                src_ref=s_out.at[k],
                dst_ref=s_in.at[k, number],
                send_sem=stat_send.at[0],
                recv_sem=stat_recv.at[k % 2],
                device_id=(clip, ph, pw),
                device_id_type=MESH,
            ).start()

    def all_stats(k, sem):
        return pltpu.make_async_copy(s_in.at[k], s_in.at[k], sem)

    def wait_stats(k):
        all_stats(k, stat_recv.at[k % 2]).wait()
        parts = [s_out[k]] + [s_in[k, i] for i in range(peers - 1)]
        while len(parts) > 1:
            parts = [
                parts[i] + parts[i + 1] if i + 1 < len(parts) else parts[i]
                for i in range(0, len(parts), 2)
            ]
        rows = jnp.concatenate([parts[0], jnp.zeros((6, c), F32)], axis=0)
        size = c // GROUPS
        place = lax.rem(lax.broadcasted_iota(jnp.int32, (8, c), 1), size)
        total = rows
        for step in range(1, size):
            total = total + jnp.where(place + step < size, pltpu.roll(rows, c - step, 1), 0.0)
            total = total + jnp.where(place >= step, pltpu.roll(rows, step, 1), 0.0)
        mean = total[0:1] / cell_count
        variance = total[1:2] / cell_count - mean * mean
        multiplier = lax.rsqrt(variance + EPSILON) * gain[k : k + 1, :]
        offset = shift[k : k + 1, :] - mean * multiplier
        return multiplier, offset

    def table(k):
        return t_last if k == convs - 1 else t.at[k % 2]

    def transform_weights(k):
        if k < 2:
            load_weights(k).wait()
        into = table(k)

        def body(dt, carry):
            for dw in range(3):
                rows = slice(dw * c, (dw + 1) * c)
                g = [wv[k, dt, dh, rows, :] for dh in range(3)]
                outer = g[0].astype(F32) + g[2].astype(F32)
                inner = g[1].astype(F32)
                values = (
                    g[0],
                    (0.5 * (outer + inner)).astype(BF16),
                    (0.5 * (outer - inner)).astype(BF16),
                    g[2],
                )
                for point in range(POINTS):
                    for e in range(2):
                        j = dw + e
                        into[point, dt, j * c : (j + 1) * c, e * c : (e + 1) * c] = values[point]
            for point in range(POINTS):
                into[point, dt, 3 * c : 4 * c, 0:c] = jnp.zeros((c, c), BF16)
                into[point, dt, 0:c, c : 2 * c] = jnp.zeros((c, c), BF16)
            return carry

        lax.fori_loop(0, 3, body, 0)

    def masked(dy, dx, values):
        return jnp.where(exists(dy, dx), values, 0.0)

    def cached_phase(k):
        for f in range(cf):
            build(
                s.at[f],
                dc.at[f],
                h,
                w,
                c,
                lambda r: cb[f, k, r * w : (r + 1) * w, :].astype(F32),
                [lambda i=i: masked(SIDE[i], 0, cr_in[i, k, f].astype(F32)) for i in range(2)],
                [lambda i=i: masked(0, SIDE[i], cc_in[i, k, f].astype(F32)) for i in range(2)],
                [lambda i=i: masked(SIDE[i // 2], SIDE[i % 2], ck_in[i, k, f]) for i in range(4)],
            )
        into = table(k)
        row = bias[k : k + 1, :]
        half = w // 2
        for o in range(fr if k % 2 else cf):
            if o < cf:
                both = row_pair(products([dc.at[p] for p in range(o, cf)], taps(into, 0, cf - o)))
            for q in range(2):
                for i in range(h // 2):
                    for e in range(2):
                        rows, lanes = slice(i * half, (i + 1) * half), slice(e * c, (e + 1) * c)
                        piece = row
                        if o < cf:
                            piece = piece + both[q][rows, lanes]
                        if k % 2:
                            at = pl.ds((2 * i + q) * w + e, half, stride=2)
                            piece = piece + res[o, at, :]
                        acc[o, q, rows, lanes] = piece

    def pack_cached(k):
        if k < 2:
            load_cache(k).wait()

        for f in range(cf):
            for side in range(2):
                top = side * (h - 1) * w
                cr_out[side, k, f] = cb[f, k, top : top + w, :]
                s[f, 0 : h * w, :] = cb[f, k].astype(F32)
                first = side * (w - 1)
                cc_out[side, k, f] = s[f, pl.ds(first, h, stride=w), :].astype(BF16)
                for low in range(2):
                    row = low * (h - 1) * w + first
                    ck_out[low * 2 + side, k, f] = s[f, row : row + 1, :]

    def settle(k):
        wait_sent(True, k)
        all_stats(k, stat_send.at[0]).wait()

    load_x.wait()

    def widen(f, carry):
        sums, squares = carry
        values = x[f].astype(F32)
        res[f] = values
        slabs = values.reshape(h * w // 8, 8, c)
        return sums + jnp.sum(slabs, axis=0), squares + jnp.sum(slabs * slabs, axis=0)

    zero = jnp.zeros((8, c), F32)
    carry = lax.fori_loop(0, fr, widen, (zero, zero))
    pack_edges(0, res)
    pack_cached(0)
    pl.semaphore_wait(barrier, peers - 1)
    send_stats(0, *carry)
    send_halo(False, 0)
    transform_weights(0)
    for k in range(1, convs):
        pack_cached(k)
    wait_sent(False, 0)
    send_halo(True, 0)
    pltpu.make_async_copy(small, small, small_sem.at[0]).wait()
    wait_halo(False, 0)
    cached_phase(0)
    last = convs - 1
    settle(0)
    for k in range(convs):
        multiplier, offset = wait_stats(k)
        wait_halo(True, k)
        if k == last:
            break
        if k == 0:
            send_halo(False, 1)
        source, target = (mid, res) if k % 2 else (res, mid)
        carry = live_phase(
            (fr, cf, h, w, c), k % 2, exists, multiplier, offset, bias[k : k + 1, :],
            source, target, (lr_in.at[k], lc_in.at[k], lk_in.at[k]),
            s, d, table(k), acc, kept.at[k], None,
        )
        send_stats(k + 1, *carry)
        pack_edges(k + 1, target)
        if k == 0:
            wait_sent(False, 1)
        send_halo(True, k + 1)
        transform_weights(k + 1)
        if k == 0:
            wait_halo(False, 1)
        cached_phase(k + 1)
        settle(k + 1)

    norm[...] = jnp.zeros_like(norm)
    norm[0:1] = multiplier
    norm[1:2] = offset
    norm[2:3] = bias[last : last + 1, :]
    hr_last[...] = lr_in[last]
    hc_last[...] = lc_in[last]
    hk_last[...] = lk_in[last]


def finish(dims, *refs):
    (mid, acc, t_last, norm_last, hr, hc, hk, kept,
     encoded, new_caches,
     s, d, out_first, out_last, kept_new, y, out_sem, kept_sem) = refs
    nh, nw, fr, cf, convs, h, w, c = dims
    exists = exists_at(nh, nw)
    copies = [
        pltpu.make_async_copy(kept.at[k], new_caches.at[:, k], kept_sem.at[k])
        for k in range(convs - 1)
    ]
    for copy in copies:
        copy.start()

    early = out_first.shape[0]

    def emit(o):
        if o < early:
            out_first[o] = y[o].astype(BF16)
        else:
            out_last[o - early] = y[o].astype(BF16)

    def send_out(source, into, sem):
        copies.append(pltpu.make_async_copy(source, into, sem))
        copies[-1].start()

    def midway():
        send_out(kept_new, new_caches.at[:, convs - 1], kept_sem.at[convs - 1])
        send_out(out_first, encoded.at[pl.ds(0, early)], out_sem.at[0])

    live_phase(
        (fr, cf, h, w, c), (convs - 1) % 2, exists, norm_last[0:1], norm_last[1:2], norm_last[2:3],
        mid, y, (hr, hc, hk), s, d, t_last, acc, kept_new, emit, midway,
    )
    send_out(out_last, encoded.at[pl.ds(early, fr - early)], out_sem.at[1])
    for copy in copies:
        copy.wait()


def local(nh, nw, frames, caches, conv_weights, conv_bias, norm_gain, norm_shift):
    fr, h, w, c = frames.shape
    cf, convs = caches.shape[:2]
    dims = (nh, nw, fr, cf, convs, h, w, c)
    peers = nh * nw
    vmem = pltpu.VMEM
    dma = pltpu.SemaphoreType.DMA
    pitch = w + 2 * LEAD
    pairs = h * w // 4
    s_shape = vmem((fr, (h + 2) * pitch, c), F32)
    d_shape = vmem((fr, POINTS, PLANES, pairs, c), BF16)
    table = (POINTS, cf + 1, PLANES * c, 2 * c)
    scratch = [
        vmem((fr, h * w, c), F32),
        vmem((fr, h * w, c), BF16),
        vmem((cf, convs, h * w, c), BF16),
        vmem((convs, 3, 3, 3 * c, c), BF16),
        s_shape,
        d_shape,
        vmem((cf, POINTS, PLANES, pairs, c), BF16),
        vmem((2,) + table, BF16),
        vmem((3, convs, c), F32),
        vmem((convs, 2, c), F32),
        vmem((convs, peers - 1, 2, c), F32),
    ]
    for _ in range(2):
        scratch += [
            vmem((convs, 2, fr, w, c), BF16),
            vmem((convs, 2, fr, h, c), BF16),
            vmem((convs, 4, fr, 1, c), F32),
        ]
    for _ in range(2):
        scratch += [
            vmem((2, convs, cf, w, c), BF16),
            vmem((2, convs, cf, h, c), BF16),
            vmem((4, convs, cf, 1, c), F32),
        ]
    scratch += [
        dma((3,)),
        dma((2,)),
        dma((1,)),
        dma((1,)),
        dma((2,)),
        dma((8,)),
        dma((4, 8)),
    ]
    anywhere = pl.BlockSpec(memory_space=pltpu.HBM)
    inside = pl.BlockSpec(memory_space=pltpu.VMEM)
    handed = [
        ((fr, h * w, c), F32),
        ((fr, 2, pairs, 2 * c), F32),
        (table, BF16),
        ((8, c), F32),
        ((2, fr, w, c), BF16),
        ((2, fr, h, c), BF16),
        ((4, fr, 1, c), F32),
        ((convs - 1, cf, h * w, c), BF16),
    ]
    state = pl.pallas_call(
        functools.partial(kernel, dims),
        out_shape=[vmem(shape, dtype) for shape, dtype in handed],
        in_specs=[anywhere] * 6,
        out_specs=[inside] * len(handed),
        scratch_shapes=scratch,
        compiler_params=pltpu.CompilerParams(
            collective_id=0, has_side_effects=True, vmem_limit_bytes=48 * 1024 * 1024
        ),
    )(
        frames.reshape(fr, h * w, c),
        caches.reshape(cf, convs, h * w, c),
        conv_weights.reshape(convs, 3, 3, 3 * c, c),
        conv_bias,
        norm_gain,
        norm_shift,
    )
    encoded, new_caches = pl.pallas_call(
        functools.partial(finish, dims),
        out_shape=(
            jax.ShapeDtypeStruct((fr, h * w, c), BF16),
            jax.ShapeDtypeStruct((cf, convs, h * w, c), BF16),
        ),
        in_specs=[inside] * len(handed),
        out_specs=(anywhere, anywhere),
        scratch_shapes=[
            s_shape,
            d_shape,
            vmem((fr - 2, h * w, c), BF16),
            vmem((2, h * w, c), BF16),
            vmem((cf, h * w, c), BF16),
            vmem((fr, h * w, c), F32),
            dma((2,)),
            dma((convs,)),
        ],
        compiler_params=pltpu.CompilerParams(vmem_limit_bytes=24 * 1024 * 1024),
    )(*state)
    return encoded.reshape(frames.shape), new_caches.reshape(caches.shape)


def solution(mesh):
    return jax.shard_map(
        functools.partial(local, mesh.shape["ha"], mesh.shape["wa"]),
        mesh=mesh,
        in_specs=(
            P("clip", "ha", "wa", None),
            P("clip", None, "ha", "wa", None),
            P(),
            P(),
            P(),
            P(),
        ),
        out_specs=(P("clip", "ha", "wa", None), P("clip", None, "ha", "wa", None)),
        check_vma=False,
    )
```

```python
import functools

import jax
import jax.numpy as jnp
from jax import lax
from jax.experimental import pallas as pl
from jax.experimental.pallas import tpu as pltpu
from jax.sharding import PartitionSpec as P

GROUPS = 32
EPSILON = 1e-06
MESH = pl.DeviceIdType.MESH
F32 = jnp.float32
BF16 = jnp.bfloat16
DIRECTIONS = [(dy, dx) for dy in (-1, 0, 1) for dx in (-1, 0, 1) if (dy, dx) != (0, 0)]
SIDE = (-1, 1)
LEAD = 8
POINTS = 4
PLANES = 4


def silu_of_half(half):
    return half + half * jnp.tanh(half)


def exists_at(nh, nw):
    ha, wa = lax.axis_index("ha"), lax.axis_index("wa")

    def exists(dy, dx):
        conds = []
        if dy:
            conds.append(ha > 0 if dy < 0 else ha < nh - 1)
        if dx:
            conds.append(wa > 0 if dx < 0 else wa < nw - 1)
        return conds[0] if len(conds) == 1 else jnp.logical_and(*conds)

    return exists


def build(s, d, h, w, c, row_of, rows, cols, ends):
    pitch = w + 2 * LEAD
    half = w // 2
    for r in range(h + 2):
        cells = rows[0]() if r == 0 else rows[1]() if r == h + 1 else row_of(r - 1)
        at = r * pitch + LEAD
        s[at : at + w, :] = cells
    for side in range(2):
        edge = LEAD - 1 + side * (w + 1)
        s[pl.ds(pitch + edge, h, stride=pitch), :] = cols[side]()
        for low in range(2):
            at = low * (h + 1) * pitch + edge
            s[at : at + 1, :] = ends[low * 2 + side]()

    def planes(r):
        return [
            s[pl.ds(r * pitch + LEAD - 1 + j, half, stride=2), :] for j in range(PLANES)
        ]

    window = [planes(0), planes(1)]
    for i in range(h // 2):
        window = window[-2:] + [planes(2 * i + 2), planes(2 * i + 3)]
        for j in range(PLANES):
            r0, r1, r2, r3 = (row[j] for row in window)
            for point, value in enumerate((r2 - r0, r1 + r2, r1 - r2, r1 - r3)):
                d[point, j, i * half : (i + 1) * half, :] = value.astype(BF16)


def taps(t, low, high):
    return lambda point: t[point, low:high].reshape(-1, t.shape[-1])


def products(pieces, right, before=None):
    m = []
    for point in range(POINTS):
        left = jnp.concatenate([p[point, j] for p in pieces for j in range(PLANES)], axis=1)
        value = jnp.dot(left, right(point), preferred_element_type=F32)
        m.append(value if before is None else value + before[point])
    return m


def row_pair(m):
    return (m[1] - m[2]) - m[0], m[1] - (m[3] - m[2])


def live_phase(dims, odd, exists, multiplier, offset, bias_row, source, target, halos, s, d, t, acc, kept, emit, midway=None):
    fr, cf, h, w, c = dims
    half = w // 2
    hr, hc, hk = halos
    multiplier, offset = 0.5 * multiplier, 0.5 * offset

    def act(values):
        return silu_of_half(values * multiplier + offset).astype(BF16)

    def masked(dy, dx, values):
        return jnp.where(exists(dy, dx), values.astype(F32), 0.0)

    def build_frame(f):
        def row_of(r):
            cells = act(source[f, r * w : (r + 1) * w, :])
            if f >= fr - cf:
                kept[f - (fr - cf), r * w : (r + 1) * w, :] = cells
            return cells.astype(F32)

        build(
            s.at[f],
            d.at[f],
            h,
            w,
            c,
            row_of,
            [lambda i=i: masked(SIDE[i], 0, act(hr[i, f].astype(F32))) for i in range(2)],
            [lambda i=i: masked(0, SIDE[i], act(hc[i, f].astype(F32))) for i in range(2)],
            [lambda i=i: masked(SIDE[i // 2], SIDE[i % 2], act(hk[i, f])) for i in range(4)],
        )

    zero = jnp.zeros((8, c), F32)
    sums, squares = zero, zero
    build_frame(0)
    before = None
    for o in range(fr):
        if o == fr - 1 and midway is not None:
            midway()
        m = products([d.at[o]], taps(t, cf, cf + 1), before)
        if o + 1 < fr:
            first = max(0, o + 1 - cf)
            before = products(
                [d.at[f] for f in range(first, o + 1)], taps(t, first + cf - o - 1, cf)
            )
            build_frame(o + 1)
        both = row_pair(m)
        for q in range(2):
            y = both[q]
            if odd or o < cf:
                y = y + acc[o, q]
            else:
                y = y + jnp.concatenate([bias_row] * 2, axis=1)
            for i in range(h // 2):
                for e in range(2):
                    piece = y[i * half : (i + 1) * half, e * c : (e + 1) * c]
                    at = pl.ds((2 * i + q) * w + e, half, stride=2)
                    if odd:
                        piece = piece.astype(BF16).astype(F32)
                    target[o, at, :] = piece
                    if emit is None:
                        slabs = piece.reshape(half // 8, 8, c)
                        sums = sums + jnp.sum(slabs, axis=0)
                        squares = squares + jnp.sum(slabs * slabs, axis=0)
        if emit is not None:
            emit(o)
    return sums, squares


def kernel(dims, *refs):
    (frames, caches, weights, bias_in, gain_in, shift_in,
     mid, acc, t_last, norm, hr_last, hc_last, hk_last, kept,
     res, x, cb, wv, s, d, dc, t, small,
     s_out, s_in,
     lr_out, lc_out, lk_out, lr_in, lc_in, lk_in,
     cr_out, cc_out, ck_out, cr_in, cc_in, ck_in,
     load_sem, weight_sem, small_sem,
     stat_send, stat_recv, halo_send, halo_recv) = refs
    nh, nw, fr, cf, convs, h, w, c = dims
    peers = nh * nw
    cell_count = fr * h * w * peers * (c // GROUPS)
    clip, ha, wa = lax.axis_index("clip"), lax.axis_index("ha"), lax.axis_index("wa")
    offsets = sorted(
        ((i, j) for i in range(nh) for j in range(nw) if (i, j) != (0, 0)),
        key=lambda ij: -sum((x % 2) * 2 + (x > 0) for x in ij),
    )
    others = [(lax.rem(ha + i, nh), lax.rem(wa + j, nw)) for i, j in offsets]
    exists = exists_at(nh, nw)
    barrier = pltpu.get_barrier_semaphore()
    for ph, pw in others:
        pl.semaphore_signal(barrier, inc=1, device_id=(clip, ph, pw), device_id_type=MESH)

    load_x = pltpu.make_async_copy(frames, x, load_sem.at[0])
    load_x.start()

    def span(k):
        return pl.ds(0, 1) if k == 0 else pl.ds(1, convs - 1)

    def load_cache(k):
        return pltpu.make_async_copy(caches.at[:, span(k)], cb.at[:, span(k)], load_sem.at[1 + k])

    def load_weights(k):
        return pltpu.make_async_copy(weights.at[span(k)], wv.at[span(k)], weight_sem.at[k])

    small_copies = [
        pltpu.make_async_copy(ref, small.at[i], small_sem.at[0])
        for i, ref in enumerate((bias_in, gain_in, shift_in))
    ]
    for copy in small_copies:
        copy.start()
    for k in range(2):
        load_cache(k).start()
        load_weights(k).start()
    bias, gain, shift = small.at[0], small.at[1], small.at[2]

    def halo_copy(live, k, dy, dx, towards):
        inbox = (1, 3)[k % 2] if live else (0, 2)[k]
        group = span(k)
        rows_out, rows_in = (lr_out, lr_in) if live else (cr_out, cr_in)
        cols_out, cols_in = (lc_out, lc_in) if live else (cc_out, cc_in)
        ends_out, ends_in = (lk_out, lk_in) if live else (ck_out, ck_in)
        if dx == 0:
            src, dst = rows_out, rows_in
            near, far = int(dy > 0), int(dy < 0)
        elif dy == 0:
            src, dst = cols_out, cols_in
            near, far = int(dx > 0), int(dx < 0)
        else:
            src, dst = ends_out, ends_in
            near = int(dy > 0) * 2 + int(dx > 0)
            far = 3 - near
        if live:
            src, dst = src.at[k, near], dst.at[k, far]
        else:
            src, dst = src.at[near, group], dst.at[far, group]
        direction = DIRECTIONS.index((dy, dx))
        back = DIRECTIONS.index((-dy, -dx))
        return pltpu.make_async_remote_copy(
            src_ref=src,
            dst_ref=dst,
            send_sem=halo_send.at[direction],
            recv_sem=halo_recv.at[inbox, back],
            device_id=(clip, ha + dy * towards, wa + dx * towards),
            device_id_type=MESH,
        )

    def pack_edges(k, field):
        for f in range(fr):
            for side in range(2):
                first = side * (w - 1)
                top = side * (h - 1) * w
                lr_out[k, side, f] = field[f, top : top + w, :].astype(BF16)
                lc_out[k, side, f] = field[f, pl.ds(first, h, stride=w), :].astype(BF16)
                for low in range(2):
                    row = low * (h - 1) * w + first
                    lk_out[k, low * 2 + side, f] = field[f, row : row + 1, :]

    def send_halo(live, k):
        for dy, dx in DIRECTIONS:

            @pl.when(exists(dy, dx))
            def _():
                halo_copy(live, k, dy, dx, 1).start()

    def wait_halo(live, k):
        for dy, dx in DIRECTIONS:

            @pl.when(exists(dy, dx))
            def _():
                halo_copy(live, k, -dy, -dx, -1).wait_recv()

    def wait_sent(live, k):
        for dy, dx in DIRECTIONS:

            @pl.when(exists(dy, dx))
            def _():
                halo_copy(live, k, dy, dx, 1).wait_send()

    def send_stats(k, sums, squares):
        s_out[k] = jnp.concatenate(
            [jnp.sum(sums, axis=0, keepdims=True), jnp.sum(squares, axis=0, keepdims=True)], axis=0
        )
        for number, (ph, pw) in enumerate(others):
            pltpu.make_async_remote_copy(
                src_ref=s_out.at[k],
                dst_ref=s_in.at[k, number],
                send_sem=stat_send.at[0],
                recv_sem=stat_recv.at[k % 2],
                device_id=(clip, ph, pw),
                device_id_type=MESH,
            ).start()

    def all_stats(k, sem):
        return pltpu.make_async_copy(s_in.at[k], s_in.at[k], sem)

    def wait_stats(k):
        all_stats(k, stat_recv.at[k % 2]).wait()
        parts = [s_out[k]] + [s_in[k, i] for i in range(peers - 1)]
        while len(parts) > 1:
            parts = [
                parts[i] + parts[i + 1] if i + 1 < len(parts) else parts[i]
                for i in range(0, len(parts), 2)
            ]
        rows = jnp.concatenate([parts[0], jnp.zeros((6, c), F32)], axis=0)
        size = c // GROUPS
        place = lax.rem(lax.broadcasted_iota(jnp.int32, (8, c), 1), size)
        total = rows
        for step in range(1, size):
            total = total + jnp.where(place + step < size, pltpu.roll(rows, c - step, 1), 0.0)
            total = total + jnp.where(place >= step, pltpu.roll(rows, step, 1), 0.0)
        mean = total[0:1] / cell_count
        variance = total[1:2] / cell_count - mean * mean
        multiplier = lax.rsqrt(variance + EPSILON) * gain[k : k + 1, :]
        offset = shift[k : k + 1, :] - mean * multiplier
        return multiplier, offset

    def table(k):
        return t_last if k == convs - 1 else t.at[k % 2]

    def transform_weights(k):
        if k < 2:
            load_weights(k).wait()
        into = table(k)

        def body(dt, carry):
            for dw in range(3):
                rows = slice(dw * c, (dw + 1) * c)
                g = [wv[k, dt, dh, rows, :] for dh in range(3)]
                outer = g[0].astype(F32) + g[2].astype(F32)
                inner = g[1].astype(F32)
                values = (
                    g[0],
                    (0.5 * (outer + inner)).astype(BF16),
                    (0.5 * (outer - inner)).astype(BF16),
                    g[2],
                )
                for point in range(POINTS):
                    for e in range(2):
                        j = dw + e
                        into[point, dt, j * c : (j + 1) * c, e * c : (e + 1) * c] = values[point]
            for point in range(POINTS):
                into[point, dt, 3 * c : 4 * c, 0:c] = jnp.zeros((c, c), BF16)
                into[point, dt, 0:c, c : 2 * c] = jnp.zeros((c, c), BF16)
            return carry

        lax.fori_loop(0, 3, body, 0)

    def masked(dy, dx, values):
        return jnp.where(exists(dy, dx), values, 0.0)

    def cached_phase(k):
        for f in range(cf):
            build(
                s.at[f],
                dc.at[f],
                h,
                w,
                c,
                lambda r: cb[f, k, r * w : (r + 1) * w, :].astype(F32),
                [lambda i=i: masked(SIDE[i], 0, cr_in[i, k, f].astype(F32)) for i in range(2)],
                [lambda i=i: masked(0, SIDE[i], cc_in[i, k, f].astype(F32)) for i in range(2)],
                [lambda i=i: masked(SIDE[i // 2], SIDE[i % 2], ck_in[i, k, f]) for i in range(4)],
            )
        into = table(k)
        row = bias[k : k + 1, :]
        half = w // 2
        for o in range(fr if k % 2 else cf):
            if o < cf:
                both = row_pair(products([dc.at[p] for p in range(o, cf)], taps(into, 0, cf - o)))
            for q in range(2):
                for i in range(h // 2):
                    for e in range(2):
                        rows, lanes = slice(i * half, (i + 1) * half), slice(e * c, (e + 1) * c)
                        piece = row
                        if o < cf:
                            piece = piece + both[q][rows, lanes]
                        if k % 2:
                            at = pl.ds((2 * i + q) * w + e, half, stride=2)
                            piece = piece + res[o, at, :]
                        acc[o, q, rows, lanes] = piece

    def pack_cached(k):
        if k < 2:
            load_cache(k).wait()

        for f in range(cf):
            for side in range(2):
                top = side * (h - 1) * w
                cr_out[side, k, f] = cb[f, k, top : top + w, :]
                s[f, 0 : h * w, :] = cb[f, k].astype(F32)
                first = side * (w - 1)
                cc_out[side, k, f] = s[f, pl.ds(first, h, stride=w), :].astype(BF16)
                for low in range(2):
                    row = low * (h - 1) * w + first
                    ck_out[low * 2 + side, k, f] = s[f, row : row + 1, :]

    def settle(k):
        wait_sent(True, k)
        all_stats(k, stat_send.at[0]).wait()

    load_x.wait()

    def widen(f, carry):
        sums, squares = carry
        values = x[f].astype(F32)
        res[f] = values
        slabs = values.reshape(h * w // 8, 8, c)
        return sums + jnp.sum(slabs, axis=0), squares + jnp.sum(slabs * slabs, axis=0)

    zero = jnp.zeros((8, c), F32)
    carry = lax.fori_loop(0, fr, widen, (zero, zero))
    pack_edges(0, res)
    pack_cached(0)
    pl.semaphore_wait(barrier, peers - 1)
    send_stats(0, *carry)
    send_halo(False, 0)
    transform_weights(0)
    for k in range(1, convs):
        pack_cached(k)
    wait_sent(False, 0)
    send_halo(True, 0)
    pltpu.make_async_copy(small, small, small_sem.at[0]).wait()
    wait_halo(False, 0)
    cached_phase(0)
    last = convs - 1
    settle(0)
    for k in range(convs):
        multiplier, offset = wait_stats(k)
        wait_halo(True, k)
        if k == last:
            break
        if k == 0:
            send_halo(False, 1)
        source, target = (mid, res) if k % 2 else (res, mid)
        carry = live_phase(
            (fr, cf, h, w, c), k % 2, exists, multiplier, offset, bias[k : k + 1, :],
            source, target, (lr_in.at[k], lc_in.at[k], lk_in.at[k]),
            s, d, table(k), acc, kept.at[k], None,
        )
        send_stats(k + 1, *carry)
        transform_weights(k + 1)
        pack_edges(k + 1, target)
        if k == 0:
            wait_sent(False, 1)
        send_halo(True, k + 1)
        if k == 0:
            wait_halo(False, 1)
        cached_phase(k + 1)
        settle(k + 1)

    norm[...] = jnp.zeros_like(norm)
    norm[0:1] = multiplier
    norm[1:2] = offset
    norm[2:3] = bias[last : last + 1, :]
    hr_last[...] = lr_in[last]
    hc_last[...] = lc_in[last]
    hk_last[...] = lk_in[last]


def finish(dims, *refs):
    (mid, acc, t_last, norm_last, hr, hc, hk, kept,
     encoded, new_caches,
     s, d, out_first, out_last, kept_new, y, out_sem, kept_sem) = refs
    nh, nw, fr, cf, convs, h, w, c = dims
    exists = exists_at(nh, nw)
    copies = [
        pltpu.make_async_copy(kept.at[k], new_caches.at[:, k], kept_sem.at[k])
        for k in range(convs - 1)
    ]
    for copy in copies:
        copy.start()

    early = out_first.shape[0]

    def emit(o):
        if o < early:
            out_first[o] = y[o].astype(BF16)
        else:
            out_last[o - early] = y[o].astype(BF16)

    def send_out(source, into, sem):
        copies.append(pltpu.make_async_copy(source, into, sem))
        copies[-1].start()

    def midway():
        send_out(kept_new, new_caches.at[:, convs - 1], kept_sem.at[convs - 1])
        send_out(out_first, encoded.at[pl.ds(0, early)], out_sem.at[0])

    live_phase(
        (fr, cf, h, w, c), (convs - 1) % 2, exists, norm_last[0:1], norm_last[1:2], norm_last[2:3],
        mid, y, (hr, hc, hk), s, d, t_last, acc, kept_new, emit, midway,
    )
    send_out(out_last, encoded.at[pl.ds(early, fr - early)], out_sem.at[1])
    for copy in copies:
        copy.wait()


def local(nh, nw, frames, caches, conv_weights, conv_bias, norm_gain, norm_shift):
    fr, h, w, c = frames.shape
    cf, convs = caches.shape[:2]
    dims = (nh, nw, fr, cf, convs, h, w, c)
    peers = nh * nw
    vmem = pltpu.VMEM
    dma = pltpu.SemaphoreType.DMA
    pitch = w + 2 * LEAD
    pairs = h * w // 4
    s_shape = vmem((fr, (h + 2) * pitch, c), F32)
    d_shape = vmem((fr, POINTS, PLANES, pairs, c), BF16)
    table = (POINTS, cf + 1, PLANES * c, 2 * c)
    scratch = [
        vmem((fr, h * w, c), F32),
        vmem((fr, h * w, c), BF16),
        vmem((cf, convs, h * w, c), BF16),
        vmem((convs, 3, 3, 3 * c, c), BF16),
        s_shape,
        d_shape,
        vmem((cf, POINTS, PLANES, pairs, c), BF16),
        vmem((2,) + table, BF16),
        vmem((3, convs, c), F32),
        vmem((convs, 2, c), F32),
        vmem((convs, peers - 1, 2, c), F32),
    ]
    for _ in range(2):
        scratch += [
            vmem((convs, 2, fr, w, c), BF16),
            vmem((convs, 2, fr, h, c), BF16),
            vmem((convs, 4, fr, 1, c), F32),
        ]
    for _ in range(2):
        scratch += [
            vmem((2, convs, cf, w, c), BF16),
            vmem((2, convs, cf, h, c), BF16),
            vmem((4, convs, cf, 1, c), F32),
        ]
    scratch += [
        dma((3,)),
        dma((2,)),
        dma((1,)),
        dma((1,)),
        dma((2,)),
        dma((8,)),
        dma((4, 8)),
    ]
    anywhere = pl.BlockSpec(memory_space=pltpu.HBM)
    inside = pl.BlockSpec(memory_space=pltpu.VMEM)
    handed = [
        ((fr, h * w, c), F32),
        ((fr, 2, pairs, 2 * c), F32),
        (table, BF16),
        ((8, c), F32),
        ((2, fr, w, c), BF16),
        ((2, fr, h, c), BF16),
        ((4, fr, 1, c), F32),
        ((convs - 1, cf, h * w, c), BF16),
    ]
    state = pl.pallas_call(
        functools.partial(kernel, dims),
        out_shape=[vmem(shape, dtype) for shape, dtype in handed],
        in_specs=[anywhere] * 6,
        out_specs=[inside] * len(handed),
        scratch_shapes=scratch,
        compiler_params=pltpu.CompilerParams(
            collective_id=0, has_side_effects=True, vmem_limit_bytes=48 * 1024 * 1024
        ),
    )(
        frames.reshape(fr, h * w, c),
        caches.reshape(cf, convs, h * w, c),
        conv_weights.reshape(convs, 3, 3, 3 * c, c),
        conv_bias,
        norm_gain,
        norm_shift,
    )
    encoded, new_caches = pl.pallas_call(
        functools.partial(finish, dims),
        out_shape=(
            jax.ShapeDtypeStruct((fr, h * w, c), BF16),
            jax.ShapeDtypeStruct((cf, convs, h * w, c), BF16),
        ),
        in_specs=[inside] * len(handed),
        out_specs=(anywhere, anywhere),
        scratch_shapes=[
            s_shape,
            d_shape,
            vmem((fr - 2, h * w, c), BF16),
            vmem((2, h * w, c), BF16),
            vmem((cf, h * w, c), BF16),
            vmem((fr, h * w, c), F32),
            dma((2,)),
            dma((convs,)),
        ],
        compiler_params=pltpu.CompilerParams(vmem_limit_bytes=24 * 1024 * 1024),
    )(*state)
    return encoded.reshape(frames.shape), new_caches.reshape(caches.shape)


def solution(mesh):
    return jax.shard_map(
        functools.partial(local, mesh.shape["ha"], mesh.shape["wa"]),
        mesh=mesh,
        in_specs=(
            P("clip", "ha", "wa", None),
            P("clip", None, "ha", "wa", None),
            P(),
            P(),
            P(),
            P(),
        ),
        out_specs=(P("clip", "ha", "wa", None), P("clip", None, "ha", "wa", None)),
        check_vma=False,
    )
```
